128 devices in a mesh: data: 1, ctxo: 2 (over core), ctx: 64 (over z, y, x).
Axes of the slice: x: 4, y: 4, z: 4, core: 2. Of those that a mesh axis runs over, the one named last changes fastest.
Arguments:
- q_seq: bfloat16 [1, 24576, 4, 128], P('data', ('ctxo', 'ctx'))
- k_seq: bfloat16 [1, 24576, 1, 128], P('data', ('ctxo', 'ctx'))
- v_seq: bfloat16 [1, 24576, 1, 128], P('data', ('ctxo', 'ctx'))
- do_seq: bfloat16 [1, 24576, 4, 128], P('data', ('ctxo', 'ctx'))
Outputs:
- output 1: bfloat16 [1, 24576, 4, 128], P('data', ('ctxo', 'ctx'))
- output 2: bfloat16 [1, 24576, 4, 128], P('data', ('ctxo', 'ctx'))
- output 3: bfloat16 [1, 24576, 1, 128], P('data', ('ctxo', 'ctx'))
- output 4: bfloat16 [1, 24576, 1, 128], P('data', ('ctxo', 'ctx'))
All inputs are finite; a program needn't handle non-finite values.
Results may differ from the reference program's by a relative error of at most 0.0106846.
Values are sent between devices in bfloat16 or wider.
A program may use at most 1 GiB of HBM per device.

```python
import math
import jax
import jax.numpy as jnp
from jax import lax

BATCH_SEQS = 1
SEQ_LEN = 24576
Q_LOCAL = 4
KV_LOCAL = 1
HEAD_DIM = 128
ROW_BLOCK = 64


def setup_inputs(seed: int = 0, part: int = 0) -> dict:
    base_key = jax.random.fold_in(jax.random.key(seed), part)
    key_q, key_k, key_v, key_d = jax.random.split(base_key, 4)
    q_shape = (BATCH_SEQS, SEQ_LEN, Q_LOCAL, HEAD_DIM)
    kv_shape = (BATCH_SEQS, SEQ_LEN, KV_LOCAL, HEAD_DIM)
    spread = math.sqrt(1.0 + math.log(max(SEQ_LEN / 256.0, 1.0)))
    q_seq = spread * jax.random.normal(key_q, q_shape, jnp.float32)
    k_seq = jax.random.normal(key_k, kv_shape, jnp.float32)
    v_seq = jax.random.normal(key_v, kv_shape, jnp.float32)
    do_seq = jax.random.normal(key_d, q_shape, jnp.float32)
    return {'q_seq': q_seq.astype(jnp.bfloat16), 'k_seq': k_seq.astype(jnp.bfloat16), 'v_seq': v_seq.astype(jnp.bfloat16), 'do_seq': do_seq.astype(jnp.bfloat16)}


def reference(q_seq, k_seq, v_seq, do_seq):
    group_size = Q_LOCAL // KV_LOCAL
    n_blocks = SEQ_LEN // ROW_BLOCK
    q_scale = 1.0 / math.sqrt(HEAD_DIM)
    blocked = (BATCH_SEQS, n_blocks, ROW_BLOCK, KV_LOCAL, group_size, HEAD_DIM)
    q_rows = jnp.moveaxis(q_seq.astype(jnp.float32).reshape(blocked), 1, 0)
    do_rows = jnp.moveaxis(do_seq.astype(jnp.float32).reshape(blocked), 1, 0)
    key_pos = lax.broadcasted_iota(jnp.int32, (1, 1, SEQ_LEN), 2)
    row_pos = lax.broadcasted_iota(jnp.int32, (ROW_BLOCK, 1, 1), 0)

    def attention(q_blocks, keys_all, vals_all):
        def one_block(block_in):
            q_blk, blk_idx = block_in
            scores = jnp.einsum('bqhgd,bkhd->bhqgk', q_blk, keys_all) * q_scale
            visible = row_pos + blk_idx * ROW_BLOCK >= key_pos
            probs_blk = jax.nn.softmax(jnp.where(visible, scores, -jnp.inf), axis=-1)
            return jnp.einsum('bhqgk,bkhd->bqhgd', probs_blk, vals_all)
        return lax.map(jax.checkpoint(one_block), (q_blocks, jnp.arange(n_blocks)))

    out_rows, pull_back = jax.vjp(attention, q_rows, k_seq.astype(jnp.float32), v_seq.astype(jnp.float32))
    dq_rows, dk_all, dv_all = pull_back(do_rows)
    q_full = (BATCH_SEQS, SEQ_LEN, Q_LOCAL, HEAD_DIM)
    out_seq = jnp.moveaxis(out_rows, 0, 1).reshape(q_full)
    dq_seq = jnp.moveaxis(dq_rows, 0, 1).reshape(q_full)
    return (out_seq.astype(jnp.bfloat16), dq_seq.astype(jnp.bfloat16), dk_all.astype(jnp.bfloat16), dv_all.astype(jnp.bfloat16))
```

```python
import functools
import math
import jax
import jax.numpy as jnp
from jax import lax
from jax.experimental import pallas as pl
from jax.experimental.pallas import tpu as pltpu
from jax.sharding import PartitionSpec as P

CTX_AXES = ('ctxo', 'ctx')
MESH = pl.DeviceIdType.MESH
f32 = jnp.float32
bf16 = jnp.bfloat16
i32 = jnp.int32

ROWS = 768
HD = 128
SUB = 48
T = 256
NT = ROWS // T
SCALE = 1.0 / math.sqrt(HD)
SCALE2 = SCALE * math.log2(math.e)
NEG = -1e30
QUAD = 4
TRIO = 3
OFFS = (1, 2, 3)
TILES = range(NT)
N_FULL = 14


def dot(a, b, ca, cb):
    return lax.dot_general(a, b, (((ca,), (cb,)), ((), ())), preferred_element_type=f32)


def tile(n):
    return slice(n * T, (n + 1) * T)


def body(q_in, k_in, v_in, do_in, o_out, dq_out, dk_out, dv_out,
         q_all, do_all, k_all, v_all, kt, vt, ot, dqt, dk, dv, cache, tb, dpb,
         m_run, l_run, lse, dd, stat_all,
         or1, or2, dqr1, dqr2, dkr1, dvr1, dk2, dv2, dkr2, dvr2, kst, vst, dk_fin, dv_fin,
         ka_ss, ka_rs, va_ss, va_rs, kx_ss, kx_rs, ky_ss, ky_rs, vy_ss, vy_rs, vx_ss, vx_rs,
         q_ss, q_rs, do_ss, do_rs, st_ss, st_rs, o1_ss, o1_rs, o2_ss, o2_rs,
         g1_ss, g1_rs, g2_ss, g2_rs, rk1_ss, rk1_rs, rv1_ss, rv1_rs, rk2_ss, rk2_rs, rv2_ss, rv2_rs,
         fk_ss, fk_rs, fv_ss, fv_rs):
    a = lax.axis_index('ctxo')
    b = lax.axis_index('ctx')
    z = b // 16
    y = (b // 4) % 4
    x = b % 4
    m_blk = 4 * y + x
    i_own = 4 * a + z
    pa = 1 - a
    par = (a + z) % 2

    def dev(a_, z_, y_, x_):
        return {'ctxo': a_, 'ctx': 16 * z_ + 4 * y_ + x_}

    def rc(src, dst, ss, rs, to):
        return pltpu.make_async_remote_copy(src_ref=src, dst_ref=dst, send_sem=ss, recv_sem=rs, device_id=to, device_id_type=MESH)

    partner = dev(pa, z, y, x)

    def got(ref, ss, rs):
        rc(ref, ref, ss, rs, partner).wait_recv()

    def sent(ref, ss, rs):
        rc(ref, ref, ss, rs, partner).wait_send()

    def zpeer(d):
        return (z + d) % 4

    def group_of(s):
        a_s = s // 2
        return a_s, 2 * (s % 2) + (a_s + a) % 2

    bar = pltpu.get_barrier_semaphore()
    for d in OFFS:
        pl.semaphore_signal(bar, inc=1, device_id=dev(a, zpeer(d), y, x), device_id_type=MESH)
        pl.semaphore_signal(bar, inc=1, device_id=dev(pa, zpeer(d), y, x), device_id_type=MESH)
        pl.semaphore_signal(bar, inc=1, device_id=dev(a, z, (y + d) % 4, x), device_id_type=MESH)
        pl.semaphore_signal(bar, inc=1, device_id=dev(a, z, y, (x + d) % 4), device_id_type=MESH)
    pl.semaphore_signal(bar, inc=1, device_id=partner, device_id_type=MESH)
    pl.semaphore_wait(bar, 13)

    k5 = k_all.reshape(4, 4, 4, SUB, HD)
    v5 = v_all.reshape(4, 4, 4, SUB, HD)

    s_me = 2 * a + z // 2
    keep = par == a
    for d in range(QUAD):
        zt = zpeer(d)
        rows = pl.ds(pl.multiple_of(SUB * zt, SUB), SUB)
        kc = rc(k_in.at[rows], k5.at[s_me, y, x], ka_ss.at[d], ka_rs.at[s_me], dev(par, zt, y, x))
        vc = rc(v_in.at[rows], v5.at[s_me, y, x], va_ss.at[d], va_rs.at[s_me], dev(par, zt, y, x))
        if d == 0:
            @pl.when(keep)
            def _():
                dst = pl.ds(pl.multiple_of(SUB * m_blk, SUB), SUB)
                k_all[s_me, dst, :] = k_in[rows, :]
                v_all[s_me, dst, :] = v_in[rows, :]

            @pl.when(jnp.logical_not(keep))
            def _():
                kc.start()
                vc.start()
        else:
            kc.start()
            vc.start()

    for d in OFFS:
        rc(q_in, q_all.at[i_own], q_ss.at[d], q_rs.at[i_own], dev(a, zpeer(d), y, x)).start()
    rc(q_in, q_all.at[i_own], q_ss.at[0], q_rs.at[i_own], partner).start()
    q_all[i_own] = q_in[...]
    do_all[i_own] = do_in[...]

    def wait_slot(s):
        a_s, z_s = group_of(s)
        mine = (a_s == a) & (z_s == z)

        @pl.when(jnp.logical_not(mine))
        def _():
            got(k5.at[s, y, x], ka_ss.at[0], ka_rs.at[s])
            got(v5.at[s, y, x], va_ss.at[0], va_rs.at[s])

    for s in range(QUAD):
        wait_slot(s)
    for d in OFFS:
        xt = dev(a, z, y, (x + d) % 4)
        yt = dev(a, z, (y + d) % 4, x)
        rc(k5.at[:, y, x], k5.at[:, y, x], kx_ss.at[d - 1], kx_rs.at[d - 1], xt).start()
        rc(v5.at[:, y, x], v5.at[:, y, x], vy_ss.at[d - 1], vy_rs.at[d - 1], yt).start()
    for d in OFFS:
        got(k5.at[:, y, (x - d) % 4], kx_ss.at[d - 1], kx_rs.at[d - 1])
        got(v5.at[:, (y - d) % 4, x], vy_ss.at[d - 1], vy_rs.at[d - 1])
    for d in OFFS:
        xt = dev(a, z, y, (x + d) % 4)
        yt = dev(a, z, (y + d) % 4, x)
        rc(k5.at[:, y], k5.at[:, y], ky_ss.at[d - 1], ky_rs.at[d - 1], yt).start()
        rc(v5.at[:, :, x], v5.at[:, :, x], vx_ss.at[d - 1], vx_rs.at[d - 1], xt).start()
    for d in OFFS:
        rc(do_in, do_all.at[i_own], do_ss.at[d], do_rs.at[i_own], dev(a, zpeer(d), y, x)).start()
    rc(do_in, do_all.at[i_own], do_ss.at[0], do_rs.at[i_own], partner).start()
    for d in OFFS:
        i_r = 4 * a + (z - d) % 4
        got(q_all.at[i_r], q_ss.at[0], q_rs.at[i_r])
        rc(q_all.at[i_r], q_all.at[i_r], q_ss.at[3 + d], q_rs.at[i_r], partner).start()

    dk[...] = jnp.zeros(dk.shape, f32)
    dv[...] = jnp.zeros(dv.shape, f32)
    dqt[...] = jnp.zeros(dqt.shape, f32)
    ot[...] = jnp.zeros(ot.shape, f32)
    m_run[...] = jnp.full(m_run.shape, NEG, f32)
    l_run[...] = jnp.zeros(l_run.shape, f32)

    for d in OFFS:
        got(k5.at[:, (y - d) % 4], ky_ss.at[d - 1], ky_rs.at[d - 1])
        got(v5.at[:, :, (x - d) % 4], vx_ss.at[d - 1], vx_rs.at[d - 1])
    for d in range(QUAD):
        i_r = 4 * pa + (z - d) % 4
        got(q_all.at[i_r], q_ss.at[0], q_rs.at[i_r])

    def transpose_kv(s, c):
        kt[s] = k_all[s].T
        vt[s] = v_all[s].T
        return c
    lax.fori_loop(0, 4, transpose_kv, 0)

    def full_count(i):
        n = jnp.int32(0)
        for s in range(QUAD):
            a_s, z_s = group_of(s)
            n = n + (4 * a_s + z_s < i).astype(i32)
        return n

    def cache_base(i):
        n = jnp.int32(0)
        for s in range(QUAD):
            a_s, z_s = group_of(s)
            n = n + jnp.maximum(i - 1 - 4 * a_s - z_s, 0)
        return n

    n_chunk = (SUB * (m_blk + 1) + T - 1) // T

    def seen(ch, ct):
        key_id = ch * T + lax.broadcasted_iota(i32, (T, T), 0)
        pos = (ct * T + lax.broadcasted_iota(i32, (1, T), 1)) // 4
        last = SUB * m_blk + jnp.clip(pos - SUB * z, -1, SUB - 1)
        return key_id <= last

    def rsum(p):
        return jnp.sum(p.reshape(p.shape[0] // 8, 8, p.shape[1]), axis=0)

    def rmax(p):
        return jnp.max(p.reshape(p.shape[0] // 8, 8, p.shape[1]), axis=0)

    def fwd_diag(i, s):
        def chunk(ch, c):
            rows = pl.ds(pl.multiple_of(ch * T, T), T)
            for ct in TILES:
                cs = tile(ct)
                t = dot(k_all[s, rows, :], q_all[i, cs, :], 1, 1) * SCALE2
                t = jnp.where(seen(ch, ct), t, -jnp.inf)
                m_old = m_run[i, :, cs]
                m_new = jnp.maximum(m_old, jnp.max(rmax(t), axis=0, keepdims=True))
                al = jnp.exp2(m_old - m_new)
                p = jnp.exp2(t - m_new)
                l_run[i, :, cs] = l_run[i, :, cs] * al + jnp.sum(rsum(p), axis=0, keepdims=True)
                ot[i, :, cs] = ot[i, :, cs] * al + dot(vt[s, :, rows], p.astype(bf16), 1, 0)
                m_run[i, :, cs] = m_new
            return c
        lax.fori_loop(0, n_chunk, chunk, 0)

    def fwd_scores(i, s, pc, ct, j, mx):
        t = dot(k_all[s, tile(j), :], q_all[i, tile(ct), :], 1, 1) * SCALE2
        cache[pc, tile(j), tile(ct)] = t
        r = rmax(t)
        return r if mx is None else jnp.maximum(mx, r)

    def fwd_full(i, n_i, base):
        @pl.when(n_i > 0)
        def _():
            mx = None
            for j in TILES:
                mx = fwd_scores(i, 0, base, 0, j, mx)

            def pair(s, mx):
                for ct in TILES:
                    cs = tile(ct)
                    s_n = s if ct < NT - 1 else jnp.minimum(s + 1, n_i - 1)
                    ct_n = (ct + 1) % NT
                    m_old = m_run[i, :, cs]
                    m_new = jnp.maximum(m_old, jnp.max(mx, axis=0, keepdims=True))
                    al = jnp.exp2(m_old - m_new)
                    mx2 = None
                    lp = None
                    o = None
                    for j in TILES:
                        mx2 = fwd_scores(i, s_n, base + s_n, ct_n, j, mx2)
                        p = jnp.exp2(cache[base + s, tile(j), cs] - m_new)
                        r = rsum(p)
                        lp = r if lp is None else lp + r
                        oj = dot(vt[s, :, tile(j)], p.astype(bf16), 1, 0)
                        o = oj if o is None else o + oj
                    l_run[i, :, cs] = l_run[i, :, cs] * al + jnp.sum(lp, axis=0, keepdims=True)
                    ot[i, :, cs] = ot[i, :, cs] * al + o
                    m_run[i, :, cs] = m_new
                    mx = mx2
                return mx
            lax.fori_loop(0, n_i, pair, mx)

    def stat_peer(off, sign):
        da, dz = divmod(off, 4)
        return (a + da) % 2, (z + sign * dz) % 4

    def fwd_step(n, c):
        i = 7 - n
        a_i = i // 4
        z_i = i % 4
        diag = (a_i + z_i) % 2 == a

        @pl.when(diag)
        def _():
            fwd_diag(i, 2 * a_i + z_i // 2)
        fwd_full(i, full_count(i), cache_base(i))

        @pl.when(n == 0)
        def _():
            for d in OFFS:
                i_r = 4 * a + (z - d) % 4
                got(do_all.at[i_r], do_ss.at[0], do_rs.at[i_r])
                rc(do_all.at[i_r], do_all.at[i_r], do_ss.at[3 + d], do_rs.at[i_r], partner).start()

        @pl.when(a_i != a)
        def _():
            got(do_all.at[i], do_ss.at[0], do_rs.at[i])
            rc(ot.at[i], or1.at[z_i], o1_ss.at[z_i], o1_rs.at[z_i], partner).start()
        d_part = jnp.sum(do_all[i].T.astype(f32) * ot[i], axis=0, keepdims=True)
        stat_all[i, i_own, 0:1, :] = m_run[i]
        stat_all[i, i_own, 1:2, :] = l_run[i]
        stat_all[i, i_own, 2:3, :] = d_part
        for off in range(1, 8):
            at, zt = stat_peer(off, 1)
            rc(stat_all.at[i, i_own], stat_all.at[i, i_own], st_ss.at[i, off - 1], st_rs.at[i, off - 1], dev(at, zt, y, x)).start()
        return c
    lax.fori_loop(0, 8, fwd_step, 0)

    def row_max(i):
        big = stat_all[i, 0, 0:1, :]
        for k in range(1, 8):
            big = jnp.maximum(big, stat_all[i, k, 0:1, :])
        return big

    def stats(i):
        for off in range(1, 8):
            af, zf = stat_peer(off, -1)
            got(stat_all.at[i, 4 * af + zf], st_ss.at[i, off - 1], st_rs.at[i, off - 1])
        big = row_max(i)
        tot = jnp.zeros((1, ROWS), f32)
        dsum = jnp.zeros((1, ROWS), f32)
        for k in range(8):
            w = jnp.exp2(stat_all[i, k, 0:1, :] - big)
            tot = tot + w * stat_all[i, k, 1:2, :]
            dsum = dsum + w * stat_all[i, k, 2:3, :]
        lse[i] = big + jnp.log(tot) * math.log2(math.e)
        dd[i] = dsum / tot

    def out_join(z_o):
        i = 4 * a + z_o
        got(or1.at[z_o], o1_ss.at[z_o], o1_rs.at[z_o])
        w_own = jnp.exp2(stat_all[i, i_own, 0:1, :] - lse[i])
        w_par = jnp.exp2(stat_all[i, 4 * pa + z, 0:1, :] - lse[i])
        for ct in TILES:
            cs = tile(ct)
            ot[i, :, cs] = ot[i, :, cs] * w_own[:, cs] + or1[z_o, :, cs] * w_par[:, cs]

        @pl.when(z_o != z)
        def _():
            h = (z_o - z) % 4 - 1
            rc(ot.at[i], or2.at[h], o2_ss.at[z_o], o2_rs.at[h], dev(a, z_o, y, x)).start()

    def dq_join(z_o):
        i = 4 * a + z_o
        got(dqr1.at[z_o], g1_ss.at[z_o], g1_rs.at[z_o])
        for ct in TILES:
            cs = tile(ct)
            dqt[i, :, cs] = dqt[i, :, cs] + dqr1[z_o, :, cs]

        @pl.when(z_o != z)
        def _():
            h = (z_o - z) % 4 - 1
            rc(dqt.at[i], dqr2.at[h], g2_ss.at[z_o], g2_rs.at[h], dev(a, z_o, y, x)).start()

    def grad_tile(i, s, t, rs, ct, slot):
        cs = tile(ct)
        p = jnp.exp2(t - lse[i, :, cs])
        ds = p * (dpb[slot] - dd[i, :, cs])
        return p.astype(bf16), ds.astype(bf16)

    def bwd_diag(i, s):
        def chunk(ch, c):
            rows = pl.ds(pl.multiple_of(ch * T, T), T)
            dv_c = None
            dk_c = None
            for ct in TILES:
                cs = tile(ct)
                t = dot(k_all[s, rows, :], q_all[i, cs, :], 1, 1) * SCALE2
                t = jnp.where(seen(ch, ct), t, -jnp.inf)
                dpb[ct] = dot(v_all[s, rows, :], do_all[i, cs, :], 1, 1)
                p, ds = grad_tile(i, s, t, rows, ct, ct)
                e = dot(p, do_all[i, cs, :], 1, 0)
                g = dot(ds, q_all[i, cs, :], 1, 0)
                dv_c = e if dv_c is None else dv_c + e
                dk_c = g if dk_c is None else dk_c + g
                dqt[i, :, cs] += dot(kt[s, :, rows], ds, 1, 0)
            dv[s, rows, :] += dv_c
            dk[s, rows, :] += dk_c
            return c
        lax.fori_loop(0, n_chunk, chunk, 0)

    def bwd_full(i, n_i, base):
        def d_scores(s, u):
            j, ct = divmod(u, NT)
            dpb[u % 3] = dot(v_all[s, tile(j), :], do_all[i, tile(ct), :], 1, 1)

        @pl.when(n_i > 0)
        def _():
            d_scores(0, 0)

            def pair(s, c):
                acc_v = None
                acc_k = None
                pend = None

                def products(u, p, ds, acc_v, acc_k):
                    j, ct = divmod(u, NT)
                    e = dot(p, do_all[i, tile(ct), :], 1, 0)
                    g = dot(ds, q_all[i, tile(ct), :], 1, 0)
                    acc_v = e if ct == 0 else acc_v + e
                    acc_k = g if ct == 0 else acc_k + g
                    dqt[i, :, tile(ct)] += dot(kt[s, :, tile(j)], ds, 1, 0)
                    if ct == NT - 1:
                        dv[s, tile(j), :] += acc_v
                        dk[s, tile(j), :] += acc_k
                    return acc_v, acc_k

                for u in range(NT * NT):
                    j, ct = divmod(u, NT)
                    if u < NT * NT - 1:
                        d_scores(s, u + 1)
                    else:
                        d_scores(jnp.minimum(s + 1, n_i - 1), 0)
                    now = grad_tile(i, s, cache[base + s, tile(j), tile(ct)], None, ct, u % 3)
                    if pend is not None:
                        acc_v, acc_k = products(u - 1, *pend, acc_v, acc_k)
                    pend = now
                products(NT * NT - 1, *pend, acc_v, acc_k)
                return c
            lax.fori_loop(0, n_i, pair, 0)

    dk5 = dk.reshape(4, 4, 4, SUB, HD)
    dv5 = dv.reshape(4, 4, 4, SUB, HD)
    dkr14 = dkr1.reshape(4, 3, 4, SUB, HD)
    dvr14 = dvr1.reshape(4, 3, 4, SUB, HD)
    dk24 = dk2.reshape(4, 4, SUB, HD)
    dv24 = dv2.reshape(4, 4, SUB, HD)

    def kv_first(s):
        for d in OFFS:
            yt = (y + d) % 4
            xt = (x + d) % 4
            rc(dk5.at[s, yt], dkr14.at[s, d - 1], rk1_ss.at[s, d - 1], rk1_rs.at[s, d - 1], dev(a, z, yt, x)).start()
            rc(dv5.at[s, :, xt], dvr14.at[s, d - 1], rv1_ss.at[s, d - 1], rv1_rs.at[s, d - 1], dev(a, z, y, xt)).start()

    def sub_rows(n):
        return pl.ds(pl.multiple_of(SUB * n, SUB), SUB)

    def kv_second(s):
        for d in OFFS:
            got(dkr14.at[s, d - 1], rk1_ss.at[s, d - 1], rk1_rs.at[s, d - 1])
            got(dvr14.at[s, d - 1], rv1_ss.at[s, d - 1], rv1_rs.at[s, d - 1])
        tot = dk[s, pl.ds(pl.multiple_of(4 * SUB * y, 4 * SUB), 4 * SUB), :]
        for d in range(TRIO):
            tot = tot + dkr1[s, d]
        dk2[s] = tot
        for n in range(QUAD):
            tot = dv[s, sub_rows(4 * n + x), :]
            for d in range(TRIO):
                tot = tot + dvr1[s, d, n * SUB:(n + 1) * SUB, :]
            dv2[s, n * SUB:(n + 1) * SUB, :] = tot
        for d in OFFS:
            yt = (y + d) % 4
            xt = (x + d) % 4
            rc(dk24.at[s, xt], dkr2.at[s, d - 1], rk2_ss.at[s, d - 1], rk2_rs.at[s, d - 1], dev(a, z, y, xt)).start()
            rc(dv24.at[s, yt], dvr2.at[s, d - 1], rv2_ss.at[s, d - 1], rv2_rs.at[s, d - 1], dev(a, z, yt, x)).start()

    def kv_third(s):
        for d in OFFS:
            got(dkr2.at[s, d - 1], rk2_ss.at[s, d - 1], rk2_rs.at[s, d - 1])
            got(dvr2.at[s, d - 1], rv2_ss.at[s, d - 1], rv2_rs.at[s, d - 1])
        tk = dk2[s, sub_rows(x), :]
        tv = dv2[s, sub_rows(y), :]
        for d in range(TRIO):
            tk = tk + dkr2[s, d]
            tv = tv + dvr2[s, d]
        kst[s] = (tk * SCALE).astype(bf16)
        vst[s] = tv.astype(bf16)
        a_s, z_s = group_of(s)
        mine = (a_s == a) & (z_s == z)
        h = (z_s - z) % 4
        rows = sub_rows(z)

        @pl.when(mine)
        def _():
            dk_fin[rows, :] = kst[s]
            dv_fin[rows, :] = vst[s]

        @pl.when(jnp.logical_not(mine))
        def _():
            rc(kst.at[s], dk_fin.at[rows], fk_ss.at[s], fk_rs.at[h], dev(a_s, z_s, y, x)).start()
            rc(vst.at[s], dv_fin.at[rows], fv_ss.at[s], fv_rs.at[h], dev(a_s, z_s, y, x)).start()

    def on_slot(i, fn):
        a_i = i // 4
        z_i = i % 4

        @pl.when((i >= 0) & (i < 8) & ((a_i + z_i) % 2 == a))
        def _():
            fn(2 * a_i + z_i // 2)

    def bwd_step(n, c):
        i = 7 - n
        a_i = i // 4
        z_i = i % 4

        @pl.when(n < 4)
        def _():
            stats(i)
            stats(i - 4)
            out_join(3 - n)

        @pl.when(n < 8)
        def _():
            bwd_full(i, full_count(i), cache_base(i))
        on_slot(i, lambda s: bwd_diag(i, s))
        on_slot(i, kv_first)

        @pl.when((n < 8) & (a_i != a))
        def _():
            rc(dqt.at[i], dqr1.at[z_i], g1_ss.at[z_i], g1_rs.at[z_i], partner).start()
        on_slot(i + 1, kv_second)
        on_slot(i + 2, kv_third)
        i1 = i + 1

        @pl.when((n >= 1) & (n <= 8) & (i1 // 4 == a))
        def _():
            dq_join(i1 % 4)
        return c
    lax.fori_loop(0, 10, bwd_step, 0)

    for h in range(TRIO):
        got(or2.at[h], o2_ss.at[0], o2_rs.at[h])
    for ct in TILES:
        cs = tile(ct)
        o_out[cs, :] = (ot[i_own, :, cs] + or2[0, :, cs] + or2[1, :, cs] + or2[2, :, cs]).T.astype(bf16)
    for h in range(TRIO):
        got(dqr2.at[h], g2_ss.at[0], g2_rs.at[h])
    for ct in TILES:
        cs = tile(ct)
        dq_out[cs, :] = ((dqt[i_own, :, cs] + dqr2[0, :, cs] + dqr2[1, :, cs] + dqr2[2, :, cs]).T * SCALE).astype(bf16)
    for h in range(QUAD):
        rows = sub_rows((z - h) % 4)

        def take():
            got(dk_fin.at[rows], fk_ss.at[0], fk_rs.at[h])
            got(dv_fin.at[rows], fv_ss.at[0], fv_rs.at[h])
        if h == 0:
            pl.when(jnp.logical_not(keep))(take)
        else:
            take()
    dk_out[...] = dk_fin[...]
    dv_out[...] = dv_fin[...]

    rows0 = pl.ds(0, SUB)
    for d in range(QUAD):
        def left():
            sent(k_in.at[rows0], ka_ss.at[d], ka_rs.at[0])
            sent(v_in.at[rows0], va_ss.at[d], va_rs.at[0])
        if d == 0:
            pl.when(jnp.logical_not(keep))(left)
        else:
            left()
    for d in range(TRIO):
        sent(k5.at[:, y, x], kx_ss.at[d], kx_rs.at[d])
        sent(v5.at[:, y, x], vy_ss.at[d], vy_rs.at[d])
        sent(k5.at[:, y], ky_ss.at[d], ky_rs.at[d])
        sent(v5.at[:, :, x], vx_ss.at[d], vx_rs.at[d])
    for d in range(7):
        sent(q_in, q_ss.at[d], q_rs.at[0])
        sent(do_in, do_ss.at[d], do_rs.at[0])

    def drain_i(i, c):
        for off in range(7):
            sent(stat_all.at[i, i_own], st_ss.at[i, off], st_rs.at[i, off])
        return c
    lax.fori_loop(0, 8, drain_i, 0)
    for n in range(QUAD):
        sent(ot.at[n], o1_ss.at[n], o1_rs.at[n])
        sent(ot.at[n], g1_ss.at[n], g1_rs.at[n])

        @pl.when(n != z)
        def _():
            sent(ot.at[n], o2_ss.at[n], o2_rs.at[0])
            sent(ot.at[n], g2_ss.at[n], g2_rs.at[0])
        for d in range(TRIO):
            sent(dkr14.at[0, 0], rk1_ss.at[n, d], rk1_rs.at[n, d])
            sent(dvr14.at[0, 0], rv1_ss.at[n, d], rv1_rs.at[n, d])
            sent(dkr2.at[0, 0], rk2_ss.at[n, d], rk2_rs.at[n, d])
            sent(dvr2.at[0, 0], rv2_ss.at[n, d], rv2_rs.at[n, d])
        a_s, z_s = group_of(n)

        @pl.when(jnp.logical_not((a_s == a) & (z_s == z)))
        def _():
            sent(kst.at[n], fk_ss.at[n], fk_rs.at[0])
            sent(vst.at[n], fv_ss.at[n], fv_rs.at[0])


def solution(mesh):
    blk_spec = P('data', CTX_AXES, None, None)

    def v(shape, dtype):
        return pltpu.VMEM(shape, dtype)

    def sem(*shape):
        return pltpu.SemaphoreType.DMA(shape)

    big = (ROWS, HD)
    scratch = [
        v((8,) + big, bf16), v((8,) + big, bf16),
        v((4,) + big, bf16), v((4,) + big, bf16),
        v((4, HD, ROWS), bf16), v((4, HD, ROWS), bf16),
        v((8, HD, ROWS), f32), v((8, HD, ROWS), f32),
        v((4,) + big, f32), v((4,) + big, f32),
        v((N_FULL, ROWS, ROWS), f32),
        v((1, 8, 128), f32), v((3, T, T), f32),
        v((8, 1, ROWS), f32), v((8, 1, ROWS), f32), v((8, 1, ROWS), f32), v((8, 1, ROWS), f32),
        v((8, 8, 3, ROWS), f32),
        v((4, HD, ROWS), f32), v((3, HD, ROWS), f32), v((4, HD, ROWS), f32), v((3, HD, ROWS), f32),
        v((4, 3, 4 * SUB, HD), f32), v((4, 3, 4 * SUB, HD), f32),
        v((4, 4 * SUB, HD), f32), v((4, 4 * SUB, HD), f32),
        v((4, 3, SUB, HD), f32), v((4, 3, SUB, HD), f32),
        v((4, SUB, HD), bf16), v((4, SUB, HD), bf16),
        v((4 * SUB, HD), bf16), v((4 * SUB, HD), bf16),
        *[sem(QUAD)] * 4, *[sem(TRIO)] * 8,
        *[sem(7), sem(8)] * 2, *[sem(8, 7)] * 2,
        *[sem(QUAD), sem(QUAD), sem(QUAD), sem(TRIO)] * 2,
        *[sem(QUAD, TRIO)] * 8, *[sem(QUAD)] * 4,
    ]
    call = pl.pallas_call(
        body,
        name='attn',
        out_shape=[jax.ShapeDtypeStruct(big, bf16), jax.ShapeDtypeStruct(big, bf16),
                   jax.ShapeDtypeStruct((4 * SUB, HD), bf16), jax.ShapeDtypeStruct((4 * SUB, HD), bf16)],
        in_specs=[pl.BlockSpec(memory_space=pltpu.VMEM)] * 4,
        out_specs=[pl.BlockSpec(memory_space=pltpu.VMEM)] * 4,
        scratch_shapes=scratch,
        compiler_params=pltpu.CompilerParams(collective_id=0, has_side_effects=True, vmem_limit_bytes=67043328),
    )

    def local_attn(q_in, k_in, v_in, do_in):
        o, dq, dk, dv = call(q_in.reshape(big), k_in.reshape(4 * SUB, HD), v_in.reshape(4 * SUB, HD), do_in.reshape(big))
        return o.reshape(q_in.shape), dq.reshape(q_in.shape), dk.reshape(k_in.shape), dv.reshape(k_in.shape)

    return jax.shard_map(local_attn, mesh=mesh, in_specs=(blk_spec,) * 4, out_specs=(blk_spec,) * 4, check_vma=False)
```

```python
import functools
import math
import jax
import jax.numpy as jnp
from jax import lax
from jax.experimental import pallas as pl
from jax.experimental.pallas import tpu as pltpu
from jax.sharding import PartitionSpec as P

CTX_AXES = ('ctxo', 'ctx')
MESH = pl.DeviceIdType.MESH
f32 = jnp.float32
bf16 = jnp.bfloat16
i32 = jnp.int32

ROWS = 768
HD = 128
SUB = 48
T = 256
NT = ROWS // T
SCALE = 1.0 / math.sqrt(HD)
SCALE2 = SCALE * math.log2(math.e)
NEG = -1e30
QUAD = 4
TRIO = 3
OFFS = (1, 2, 3)
TILES = range(NT)
N_FULL = 14


def dot(a, b, ca, cb):
    return lax.dot_general(a, b, (((ca,), (cb,)), ((), ())), preferred_element_type=f32)


def tile(n):
    return slice(n * T, (n + 1) * T)


def body(q_in, k_in, v_in, do_in, o_out, dq_out, dk_out, dv_out,
         q_all, do_all, k_all, v_all, kt, vt, ot, dqt, dk, dv, cache, scb, dpb, mx_run,
         m_run, l_run, lse, dd, stat_all,
         or1, or2, dqr1, dqr2, dkr1, dvr1, dk2, dv2, dkr2, dvr2, kst, vst, dk_fin, dv_fin,
         ka_ss, ka_rs, va_ss, va_rs, kx_ss, kx_rs, vy_ss, vy_rs, ky_ss, ky_rs, vx_ss, vx_rs,
         q_ss, q_rs, do_ss, do_rs, st_ss, st_rs, o1_ss, o1_rs, o2_ss, o2_rs,
         g1_ss, g1_rs, g2_ss, g2_rs, rk1_ss, rk1_rs, rv1_ss, rv1_rs, rk2_ss, rk2_rs, rv2_ss, rv2_rs,
         fk_ss, fk_rs, fv_ss, fv_rs):
    a = lax.axis_index('ctxo')
    b = lax.axis_index('ctx')
    z = b // 16
    y = (b // 4) % 4
    x = b % 4
    m_blk = 4 * y + x
    i_own = 4 * a + z
    pa = 1 - a
    par = (a + z) % 2

    def dev(a_, z_, y_, x_):
        return {'ctxo': a_, 'ctx': 16 * z_ + 4 * y_ + x_}

    def rc(src, dst, ss, rs, to):
        return pltpu.make_async_remote_copy(src_ref=src, dst_ref=dst, send_sem=ss, recv_sem=rs, device_id=to, device_id_type=MESH)

    partner = dev(pa, z, y, x)

    def got(ref, ss, rs):
        rc(ref, ref, ss, rs, partner).wait_recv()

    def sent(ref, ss, rs):
        rc(ref, ref, ss, rs, partner).wait_send()

    def zpeer(d):
        return (z + d) % 4

    def sub_rows(n):
        return pl.ds(pl.multiple_of(SUB * n, SUB), SUB)

    def group_of(s):
        a_s = s // 2
        return a_s, 2 * (s % 2) + (a_s + a) % 2

    bar = pltpu.get_barrier_semaphore()

    def hello(to):
        pl.semaphore_signal(bar, inc=1, device_id=to, device_id_type=MESH)

    hello(partner)
    for d in OFFS:
        hello(dev(a, zpeer(d), y, x))
        hello(dev(pa, zpeer(d), y, x))
        hello(dev(a, z, (y + d) % QUAD, x))
        hello(dev(a, z, y, (x + d) % QUAD))
    pl.semaphore_wait(bar, 13)

    k5 = k_all.reshape(4, 4, 4, SUB, HD)
    v5 = v_all.reshape(4, 4, 4, SUB, HD)

    s_me = 2 * a + z // 2
    keep = par == a
    for d in range(QUAD):
        rows = sub_rows(zpeer(d))
        kc = rc(k_in.at[rows], k5.at[s_me, y, x], ka_ss.at[d], ka_rs.at[s_me], dev(par, zpeer(d), y, x))
        vc = rc(v_in.at[rows], v5.at[s_me, y, x], va_ss.at[d], va_rs.at[s_me], dev(par, zpeer(d), y, x))
        if d == 0:
            @pl.when(keep)
            def _():
                k_all[s_me, sub_rows(m_blk), :] = k_in[rows, :]
                v_all[s_me, sub_rows(m_blk), :] = v_in[rows, :]

            @pl.when(jnp.logical_not(keep))
            def _():
                kc.start()
                vc.start()
        else:
            kc.start()
            vc.start()

    rc(q_in, q_all.at[i_own], q_ss.at[0], q_rs.at[i_own], partner).start()
    for d in OFFS:
        rc(q_in, q_all.at[i_own], q_ss.at[d], q_rs.at[i_own], dev(a, zpeer(d), y, x)).start()
    q_all[i_own] = q_in[...]
    do_all[i_own] = do_in[...]
    dk[...] = jnp.zeros(dk.shape, f32)
    dv[...] = jnp.zeros(dv.shape, f32)

    def kv_share():
        for s in range(QUAD):
            a_s, z_s = group_of(s)

            @pl.when(jnp.logical_not((a_s == a) & (z_s == z)))
            def _():
                got(k5.at[s, y, x], ka_ss.at[0], ka_rs.at[s])
                got(v5.at[s, y, x], va_ss.at[0], va_rs.at[s])
        for d in OFFS:
            rc(k5.at[:, y, x], k5.at[:, y, x], kx_ss.at[d - 1], kx_rs.at[d - 1], dev(a, z, y, (x + d) % QUAD)).start()
            rc(v5.at[:, y, x], v5.at[:, y, x], vy_ss.at[d - 1], vy_rs.at[d - 1], dev(a, z, (y + d) % QUAD, x)).start()

    def kv_spread():
        for d in OFFS:
            got(k5.at[:, y, (x - d) % QUAD], kx_ss.at[d - 1], kx_rs.at[d - 1])
            got(v5.at[:, (y - d) % QUAD, x], vy_ss.at[d - 1], vy_rs.at[d - 1])
        for s in range(QUAD):
            for d in OFFS:
                rc(k5.at[s, y], k5.at[s, y], ky_ss.at[s, d - 1], ky_rs.at[s, d - 1], dev(a, z, (y + d) % QUAD, x)).start()
                rc(v5.at[s, :, x], v5.at[s, :, x], vx_ss.at[s, d - 1], vx_rs.at[s, d - 1], dev(a, z, y, (x + d) % QUAD)).start()

    def kv_ready(s):
        for d in OFFS:
            got(k5.at[s, (y - d) % QUAD], ky_ss.at[s, d - 1], ky_rs.at[s, d - 1])
            got(v5.at[s, :, (x - d) % QUAD], vx_ss.at[s, d - 1], vx_rs.at[s, d - 1])
        kt[s] = k_all[s].T
        vt[s] = v_all[s].T

    kv_share()
    dqt[...] = jnp.zeros(dqt.shape, f32)
    ot[...] = jnp.zeros(ot.shape, f32)
    kv_spread()
    rc(do_in, do_all.at[i_own], do_ss.at[0], do_rs.at[i_own], partner).start()
    for d in OFFS:
        rc(do_in, do_all.at[i_own], do_ss.at[d], do_rs.at[i_own], dev(a, zpeer(d), y, x)).start()
    m_run[...] = jnp.full(m_run.shape, NEG, f32)
    l_run[...] = jnp.zeros(l_run.shape, f32)

    def hand_on(full, ss, rs, d):
        i_r = 4 * a + (z - d) % QUAD
        got(full.at[i_r], ss.at[0], rs.at[i_r])
        rc(full.at[i_r], full.at[i_r], ss.at[3 + d], rs.at[i_r], partner).start()

    def q_ready(d):
        i_r = 4 * pa + (z - d) % QUAD
        got(q_all.at[i_r], q_ss.at[0], q_rs.at[i_r])

    hand_on(q_all, q_ss, q_rs, 1)
    hand_on(q_all, q_ss, q_rs, 3)

    def g_of(s):
        a_s, z_s = group_of(s)
        return 4 * a_s + z_s

    def full_count(i):
        n = jnp.int32(0)
        for s in range(QUAD):
            n = n + (g_of(s) < i).astype(i32)
        return n

    def cache_at(i, s):
        n = i - g_of(s) - 1
        for r in OFFS:
            n = n + (r <= s) * (7 - g_of(r - 1))
        return n

    def seen(j, ct):
        key_id = j * T + lax.broadcasted_iota(i32, (T, T), 0)
        pos = (ct * T + lax.broadcasted_iota(i32, (1, T), 1)) // 4
        last = SUB * m_blk + jnp.clip(pos - SUB * z, -1, SUB - 1)
        return key_id <= last

    def rsum(p):
        return jnp.sum(p.reshape(p.shape[0] // 8, 8, p.shape[1]), axis=0)

    def rmax(p):
        return jnp.max(p.reshape(p.shape[0] // 8, 8, p.shape[1]), axis=0)

    def fwd_scores(i, s, pc, ct, j, mx, masked=False):
        t = dot(k_all[s, tile(j), :], q_all[i, tile(ct), :], 1, 1) * SCALE2
        if masked:
            t = jnp.where(seen(j, ct), t, -jnp.inf)
        cache[pc, tile(j), tile(ct)] = t
        r = rmax(t)
        return r if mx is None else jnp.maximum(mx, r)

    def fwd_pair(i, s, pc, mx, i_n, pc_n, masked=False):
        for ct in TILES:
            cs = tile(ct)
            last = ct == NT - 1
            nxt = (i_n, s, pc_n, 0) if last else (i, s, pc, ct + 1)
            m_old = m_run[i, :, cs]
            m_new = jnp.maximum(m_old, jnp.max(mx, axis=0, keepdims=True))
            al = jnp.exp2(m_old - m_new)
            mx = None
            lp = None
            o = None
            for j in TILES:
                if not (masked and last):
                    mx = fwd_scores(*nxt, j, mx, masked)
                p = jnp.exp2(cache[pc, tile(j), cs] - m_new)
                r = rsum(p)
                lp = r if lp is None else lp + r
                oj = dot(vt[s, :, tile(j)], p.astype(bf16), 1, 0)
                o = oj if o is None else o + oj
            l_run[i, :, cs] = l_run[i, :, cs] * al + jnp.sum(lp, axis=0, keepdims=True)
            ot[i, :, cs] = ot[i, :, cs] * al + o
            m_run[i, :, cs] = m_new
        return mx

    def nth(t):
        r = t // 2
        d = r + (r >= 2) * (1 - 2 * (r - 2))
        return 4 * ((a + t) % 2) + (z + d) % QUAD

    def fwd_slot(s):
        kv_ready(s)
        g = g_of(s)

        def after(t):
            n = jnp.int32(8)
            for k in range(7, -1, -1):
                n = jnp.where((k > t) & (nth(k) > g), k, n)
            return n

        @pl.when(s == 0)
        def _():
            for d in (0, 1, 3):
                q_ready(d)
        t0 = after(jnp.int32(-1))

        @pl.when(t0 < 8)
        def _():
            mx = None
            for j in TILES:
                mx = fwd_scores(nth(t0), s, cache_at(nth(t0), s), 0, j, mx)
            mx_run[...] = mx

        def pair(t, c):
            @pl.when((s == 0) & (t == 3))
            def _():
                hand_on(q_all, q_ss, q_rs, 2)

            @pl.when((s == 0) & (t == 5))
            def _():
                q_ready(2)

            @pl.when(nth(t) > g)
            def _():
                i = nth(t)
                t_n = after(t)
                i_n = jnp.where(t_n < 8, nth(t_n), i)
                mx_run[...] = fwd_pair(i, s, cache_at(i, s), mx_run[...], i_n, cache_at(i_n, s))
            return c
        lax.fori_loop(0, 8, pair, 0)
        mx = None
        for j in TILES:
            mx = fwd_scores(g, s, N_FULL, 0, j, mx, True)
        fwd_pair(g, s, N_FULL, mx, None, None, True)

    def stat_peer(off, sign):
        da, dz = divmod(off, 4)
        return (a + da) % 2, (z + sign * dz) % QUAD

    def fwd_done(i, c):
        a_i = i // 4
        z_i = i % QUAD

        @pl.when(a_i != a)
        def _():
            got(do_all.at[i], do_ss.at[0], do_rs.at[i])
        d_part = jnp.sum(do_all[i].T.astype(f32) * ot[i], axis=0, keepdims=True)
        stat_all[i, i_own, 0:1, :] = m_run[i]
        stat_all[i, i_own, 1:2, :] = l_run[i]
        stat_all[i, i_own, 2:3, :] = d_part
        for off in range(1, 8):
            at, zt = stat_peer(off, 1)
            rc(stat_all.at[i, i_own], stat_all.at[i, i_own], st_ss.at[i, off - 1], st_rs.at[i, off - 1], dev(at, zt, y, x)).start()

        @pl.when(a_i != a)
        def _():
            rc(ot.at[i], or1.at[z_i], o1_ss.at[z_i], o1_rs.at[z_i], partner).start()
        return c

    def pair_max(i, z_):
        return jnp.maximum(stat_all[i, z_, 0:1, :], stat_all[i, 4 + z_, 0:1, :])

    def out_join(z_o):
        i = 4 * a + z_o
        got(or1.at[z_o], o1_ss.at[z_o], o1_rs.at[z_o])
        got(stat_all.at[i, 4 * pa + z], st_ss.at[i, 3], st_rs.at[i, 3])
        top = pair_max(i, z)
        w_own = jnp.exp2(stat_all[i, i_own, 0:1, :] - top)
        w_par = jnp.exp2(stat_all[i, 4 * pa + z, 0:1, :] - top)
        for ct in TILES:
            cs = tile(ct)
            ot[i, :, cs] = ot[i, :, cs] * w_own[:, cs] + or1[z_o, :, cs] * w_par[:, cs]

        @pl.when(z_o != z)
        def _():
            h = (z_o - z) % QUAD - 1
            rc(ot.at[i], or2.at[h], o2_ss.at[z_o], o2_rs.at[h], dev(a, z_o, y, x)).start()

    def slot_step(s, c):
        fwd_slot(s)

        @pl.when(s == 1)
        def _():
            for d in (1, 3, 2):
                hand_on(do_all, do_ss, do_rs, d)

        @pl.when(s == 2)
        def _():
            lax.fori_loop(0, g_of(3), fwd_done, 0)

        @pl.when(s == 3)
        def _():
            lax.fori_loop(g_of(3), 8, fwd_done, 0)
        return c
    lax.fori_loop(0, 4, slot_step, 0)

    def row_max(i):
        big = stat_all[i, 0, 0:1, :]
        for k in range(1, 8):
            big = jnp.maximum(big, stat_all[i, k, 0:1, :])
        return big

    def stats(i):
        for off in range(1, 8):
            af, zf = stat_peer(off, -1)

            def take():
                got(stat_all.at[i, 4 * af + zf], st_ss.at[i, off - 1], st_rs.at[i, off - 1])
            if off == 4:
                pl.when(i // 4 != a)(take)
            else:
                take()
        big = row_max(i)
        tot = jnp.zeros((1, ROWS), f32)
        dsum = jnp.zeros((1, ROWS), f32)
        for k in range(8):
            w = jnp.exp2(stat_all[i, k, 0:1, :] - big)
            tot = tot + w * stat_all[i, k, 1:2, :]
            dsum = dsum + w * stat_all[i, k, 2:3, :]
        lse[i] = big + jnp.log(tot) * math.log2(math.e)
        dd[i] = dsum / tot

    def dq_join(z_o):
        i = 4 * a + z_o
        got(dqr1.at[z_o], g1_ss.at[z_o], g1_rs.at[z_o])
        for ct in TILES:
            cs = tile(ct)
            dqt[i, :, cs] = dqt[i, :, cs] + dqr1[z_o, :, cs]

        @pl.when(z_o != z)
        def _():
            h = (z_o - z) % 4 - 1
            rc(dqt.at[i], dqr2.at[h], g2_ss.at[z_o], g2_rs.at[h], dev(a, z_o, y, x)).start()

    def bwd_scores(i, s, u, masked):
        j, ct = divmod(u, NT)
        dpb[u % TRIO] = dot(v_all[s, tile(j), :], do_all[i, tile(ct), :], 1, 1)
        if masked:
            t = dot(k_all[s, tile(j), :], q_all[i, tile(ct), :], 1, 1) * SCALE2
            scb[u % TRIO] = jnp.where(seen(j, ct), t, -jnp.inf)

    def bwd_pair(i, s, pc, s_n, masked=False):
        acc_v = None
        acc_k = None
        pend = None

        def products(u, p, ds, acc_v, acc_k):
            j, ct = divmod(u, NT)
            e = dot(p, do_all[i, tile(ct), :], 1, 0)
            g = dot(ds, q_all[i, tile(ct), :], 1, 0)
            acc_v = e if ct == 0 else acc_v + e
            acc_k = g if ct == 0 else acc_k + g
            dqt[i, :, tile(ct)] += dot(kt[s, :, tile(j)], ds, 1, 0)
            if ct == NT - 1:
                dv[s, tile(j), :] += acc_v
                dk[s, tile(j), :] += acc_k
            return acc_v, acc_k

        n_u = NT * NT
        for u in range(n_u):
            j, ct = divmod(u, NT)
            if u < n_u - 1:
                bwd_scores(i, s, u + 1, masked)
            else:
                bwd_scores(i, s_n, 0, False)
            t = scb[u % TRIO] if masked else cache[pc, tile(j), tile(ct)]
            p = jnp.exp2(t - lse[i, :, tile(ct)])
            ds = p * (dpb[u % TRIO] - dd[i, :, tile(ct)])
            now = p.astype(bf16), ds.astype(bf16)
            if pend is not None:
                acc_v, acc_k = products(u - 1, *pend, acc_v, acc_k)
            pend = now
        products(n_u - 1, *pend, acc_v, acc_k)

    def bwd_block(i):
        n_i = full_count(i)
        diag = (i // 4 + i) % 2 == a
        s_d = 2 * (i // 4) + i % QUAD // 2

        @pl.when(diag)
        def _():
            bwd_scores(i, s_d, 0, True)
            bwd_pair(i, s_d, N_FULL, 0, True)

        @pl.when(jnp.logical_not(diag))
        def _():
            bwd_scores(i, 0, 0, False)

        def pair(s, c):
            bwd_pair(i, s, cache_at(i, s), jnp.minimum(s + 1, 3))
            return c
        lax.fori_loop(0, n_i, pair, 0)

    dk5 = dk.reshape(4, 4, 4, SUB, HD)
    dv5 = dv.reshape(4, 4, 4, SUB, HD)
    dkr14 = dkr1.reshape(4, 3, 4, SUB, HD)
    dvr14 = dvr1.reshape(4, 3, 4, SUB, HD)
    dk24 = dk2.reshape(4, 4, SUB, HD)
    dv24 = dv2.reshape(4, 4, SUB, HD)

    def kv_first(s):
        for d in OFFS:
            yt = (y + d) % 4
            xt = (x + d) % 4
            rc(dk5.at[s, yt], dkr14.at[s, d - 1], rk1_ss.at[s, d - 1], rk1_rs.at[s, d - 1], dev(a, z, yt, x)).start()
            rc(dv5.at[s, :, xt], dvr14.at[s, d - 1], rv1_ss.at[s, d - 1], rv1_rs.at[s, d - 1], dev(a, z, y, xt)).start()

    def kv_second(s):
        for d in OFFS:
            got(dkr14.at[s, d - 1], rk1_ss.at[s, d - 1], rk1_rs.at[s, d - 1])
            got(dvr14.at[s, d - 1], rv1_ss.at[s, d - 1], rv1_rs.at[s, d - 1])
        tot = dk[s, pl.ds(pl.multiple_of(4 * SUB * y, 4 * SUB), 4 * SUB), :]
        for d in range(TRIO):
            tot = tot + dkr1[s, d]
        dk2[s] = tot
        for n in range(QUAD):
            tot = dv[s, sub_rows(4 * n + x), :]
            for d in range(TRIO):
                tot = tot + dvr1[s, d, n * SUB:(n + 1) * SUB, :]
            dv2[s, n * SUB:(n + 1) * SUB, :] = tot
        for d in OFFS:
            yt = (y + d) % 4
            xt = (x + d) % 4
            rc(dk24.at[s, xt], dkr2.at[s, d - 1], rk2_ss.at[s, d - 1], rk2_rs.at[s, d - 1], dev(a, z, y, xt)).start()
            rc(dv24.at[s, yt], dvr2.at[s, d - 1], rv2_ss.at[s, d - 1], rv2_rs.at[s, d - 1], dev(a, z, yt, x)).start()

    def kv_third(s):
        for d in OFFS:
            got(dkr2.at[s, d - 1], rk2_ss.at[s, d - 1], rk2_rs.at[s, d - 1])
            got(dvr2.at[s, d - 1], rv2_ss.at[s, d - 1], rv2_rs.at[s, d - 1])
        tk = dk2[s, sub_rows(x), :]
        tv = dv2[s, sub_rows(y), :]
        for d in range(TRIO):
            tk = tk + dkr2[s, d]
            tv = tv + dvr2[s, d]
        kst[s] = (tk * SCALE).astype(bf16)
        vst[s] = tv.astype(bf16)
        a_s, z_s = group_of(s)
        mine = (a_s == a) & (z_s == z)
        h = (z_s - z) % 4
        rows = sub_rows(z)

        @pl.when(mine)
        def _():
            dk_fin[rows, :] = kst[s]
            dv_fin[rows, :] = vst[s]

        @pl.when(jnp.logical_not(mine))
        def _():
            rc(kst.at[s], dk_fin.at[rows], fk_ss.at[s], fk_rs.at[h], dev(a_s, z_s, y, x)).start()
            rc(vst.at[s], dv_fin.at[rows], fv_ss.at[s], fv_rs.at[h], dev(a_s, z_s, y, x)).start()

    def on_slots(n, delay, fn, late):
        for s in range(QUAD):
            when = (7, 5, 3, 1)[s] + a * ((6, 5, 4, 2)[s] - (7, 5, 3, 1)[s]) + delay
            pl.when((when == n) | ((n == 8) & (when > 7)) if late else when == n)(functools.partial(fn, s))

    def bwd_step(n, c):
        i = 7 - n + ((n >= 1) & (n <= 4)).astype(i32) - 4 * (n == 0).astype(i32)
        a_i = i // 4
        z_i = i % QUAD
        stats(i)
        bwd_block(i)

        @pl.when(a_i != a)
        def _():
            rc(dqt.at[i], dqr1.at[z_i], g1_ss.at[z_i], g1_rs.at[z_i], partner).start()
        on_slots(n, 0, kv_first, False)

        @pl.when((n == 0) & (a == 1))
        def _():
            out_join(3)
            out_join(2)

        @pl.when(((a == 0) & (n == 1)) | ((a == 1) & (n == 2)))
        def _():
            dq_join(3)

        @pl.when(((a == 0) & (n == 6)) | ((a == 1) & (n == 3)))
        def _():
            dq_join(2)

        @pl.when(((a == 0) & (n == 7)) | ((a == 1) & (n == 4)))
        def _():
            dq_join(1)

        @pl.when((a == 1) & (n == 5))
        def _():
            dq_join(0)
        on_slots(n, 2, kv_second, False)
        on_slots(n, 4, kv_third, False)
        return c

    @pl.when(a == 0)
    def _():
        for n in (3, 2, 1, 0):
            out_join(n)

    @pl.when(a == 1)
    def _():
        out_join(1)
        out_join(0)
    lax.fori_loop(0, 8, bwd_step, 0)

    @pl.when(a == 0)
    def _():
        dq_join(0)

    for h in range(TRIO):
        got(or2.at[h], o2_ss.at[0], o2_rs.at[h])
    w_z = [jnp.exp2(pair_max(i_own, (z - h) % QUAD) - lse[i_own]) for h in range(QUAD)]
    for ct in TILES:
        cs = tile(ct)
        o = ot[i_own, :, cs] * w_z[0][:, cs]
        for h in OFFS:
            o = o + or2[h - 1, :, cs] * w_z[h][:, cs]
        o_out[cs, :] = o.T.astype(bf16)
    on_slots(8, 2, kv_second, True)
    on_slots(8, 4, kv_third, True)
    for h in range(TRIO):
        got(dqr2.at[h], g2_ss.at[0], g2_rs.at[h])
    for ct in TILES:
        cs = tile(ct)
        dq_out[cs, :] = ((dqt[i_own, :, cs] + dqr2[0, :, cs] + dqr2[1, :, cs] + dqr2[2, :, cs]).T * SCALE).astype(bf16)
    for h in range(QUAD):
        rows = sub_rows((z - h) % 4)

        def take():
            got(dk_fin.at[rows], fk_ss.at[0], fk_rs.at[h])
            got(dv_fin.at[rows], fv_ss.at[0], fv_rs.at[h])
        if h == 0:
            pl.when(jnp.logical_not(keep))(take)
        else:
            take()
    dk_out[...] = dk_fin[...]
    dv_out[...] = dv_fin[...]

    rows0 = pl.ds(0, SUB)
    for d in range(QUAD):
        def left():
            sent(k_in.at[rows0], ka_ss.at[d], ka_rs.at[0])
            sent(v_in.at[rows0], va_ss.at[d], va_rs.at[0])
        if d == 0:
            pl.when(jnp.logical_not(keep))(left)
        else:
            left()
        for h in range(TRIO):
            sent(k5.at[d, y], ky_ss.at[d, h], ky_rs.at[d, h])
            sent(v5.at[d, :, x], vx_ss.at[d, h], vx_rs.at[d, h])
    for d in range(TRIO):
        sent(k5.at[:, y, x], kx_ss.at[d], kx_rs.at[d])
        sent(v5.at[:, y, x], vy_ss.at[d], vy_rs.at[d])
    for d in range(7):
        sent(q_in, q_ss.at[d], q_rs.at[0])
        sent(do_in, do_ss.at[d], do_rs.at[0])

    def drain_i(i, c):
        for off in range(7):
            sent(stat_all.at[i, i_own], st_ss.at[i, off], st_rs.at[i, off])
        return c
    lax.fori_loop(0, 8, drain_i, 0)
    for n in range(QUAD):
        sent(ot.at[n], o1_ss.at[n], o1_rs.at[n])
        sent(ot.at[n], g1_ss.at[n], g1_rs.at[n])

        @pl.when(n != z)
        def _():
            sent(ot.at[n], o2_ss.at[n], o2_rs.at[0])
            sent(ot.at[n], g2_ss.at[n], g2_rs.at[0])
        for d in range(TRIO):
            sent(dkr14.at[0, 0], rk1_ss.at[n, d], rk1_rs.at[n, d])
            sent(dvr14.at[0, 0], rv1_ss.at[n, d], rv1_rs.at[n, d])
            sent(dkr2.at[0, 0], rk2_ss.at[n, d], rk2_rs.at[n, d])
            sent(dvr2.at[0, 0], rv2_ss.at[n, d], rv2_rs.at[n, d])
        a_s, z_s = group_of(n)

        @pl.when(jnp.logical_not((a_s == a) & (z_s == z)))
        def _():
            sent(kst.at[n], fk_ss.at[n], fk_rs.at[0])
            sent(vst.at[n], fv_ss.at[n], fv_rs.at[0])


def solution(mesh):
    blk_spec = P('data', CTX_AXES, None, None)

    def v(shape, dtype):
        return pltpu.VMEM(shape, dtype)

    def sem(*shape):
        return pltpu.SemaphoreType.DMA(shape)

    big = (ROWS, HD)
    scratch = [
        v((8,) + big, bf16), v((8,) + big, bf16),
        v((4,) + big, bf16), v((4,) + big, bf16),
        v((4, HD, ROWS), bf16), v((4, HD, ROWS), bf16),
        v((8, HD, ROWS), f32), v((8, HD, ROWS), f32),
        v((4,) + big, f32), v((4,) + big, f32),
        v((N_FULL + 1, ROWS, ROWS), f32),
        v((3, T, T), f32), v((3, T, T), f32),
        v((8, T), f32),
        v((8, 1, ROWS), f32), v((8, 1, ROWS), f32), v((8, 1, ROWS), f32), v((8, 1, ROWS), f32),
        v((8, 8, 3, ROWS), f32),
        v((4, HD, ROWS), f32), v((3, HD, ROWS), f32), v((4, HD, ROWS), f32), v((3, HD, ROWS), f32),
        v((4, 3, 4 * SUB, HD), f32), v((4, 3, 4 * SUB, HD), f32),
        v((4, 4 * SUB, HD), f32), v((4, 4 * SUB, HD), f32),
        v((4, 3, SUB, HD), f32), v((4, 3, SUB, HD), f32),
        v((4, SUB, HD), bf16), v((4, SUB, HD), bf16),
        v((4 * SUB, HD), bf16), v((4 * SUB, HD), bf16),
        *[sem(QUAD)] * 4, *[sem(TRIO)] * 4, *[sem(QUAD, TRIO)] * 4,
        *[sem(7), sem(8)] * 2, *[sem(8, 7)] * 2,
        *[sem(QUAD), sem(QUAD), sem(QUAD), sem(TRIO)] * 2,
        *[sem(QUAD, TRIO)] * 8, *[sem(QUAD)] * 4,
    ]
    call = pl.pallas_call(
        body,
        name='attn',
        out_shape=[jax.ShapeDtypeStruct(big, bf16), jax.ShapeDtypeStruct(big, bf16),
                   jax.ShapeDtypeStruct((4 * SUB, HD), bf16), jax.ShapeDtypeStruct((4 * SUB, HD), bf16)],
        in_specs=[pl.BlockSpec(memory_space=pltpu.VMEM)] * 4,
        out_specs=[pl.BlockSpec(memory_space=pltpu.VMEM)] * 4,
        scratch_shapes=scratch,
        compiler_params=pltpu.CompilerParams(collective_id=0, has_side_effects=True, vmem_limit_bytes=67043328),
    )

    def local_attn(q_in, k_in, v_in, do_in):
        o, dq, dk, dv = call(q_in.reshape(big), k_in.reshape(4 * SUB, HD), v_in.reshape(4 * SUB, HD), do_in.reshape(big))
        return o.reshape(q_in.shape), dq.reshape(q_in.shape), dk.reshape(k_in.shape), dv.reshape(k_in.shape)

    return jax.shard_map(local_attn, mesh=mesh, in_specs=(blk_spec,) * 4, out_specs=(blk_spec,) * 4, check_vma=False)
```

```python
import functools
import math
import jax
import jax.numpy as jnp
from jax import lax
from jax.experimental import pallas as pl
from jax.experimental.pallas import tpu as pltpu
from jax.sharding import PartitionSpec as P

CTX_AXES = ('ctxo', 'ctx')
MESH = pl.DeviceIdType.MESH
f32 = jnp.float32
bf16 = jnp.bfloat16
i32 = jnp.int32

Z = 4
G = 8
HD = 128
SUB = 48
BLK = Z * SUB
ROWS = Z * BLK
HALF = ROWS // 2
T = 256
NT = ROWS // T
TILES = range(NT)
QUAD = range(Z)
OFFS = (1, 2, 3)
NEAR = (1, 3)
SCALE = 1.0 / math.sqrt(HD)
SCALE2 = SCALE * math.log2(math.e)
NEG = -1e30
N_FULL = 14
LAST = G - 1

KINDS = (('ka', Z), ('va', Z), ('kx', Z), ('vy', Z), ('ky', Z * Z), ('vx', Z * Z),
         ('q', G), ('qh', Z), ('qf', Z), ('do', G), ('doh', Z), ('dof', Z), ('in', Z),
         ('st', Z), ('sz', Z * Z), ('ld', G), ('o', Z), ('oz', Z), ('g', Z), ('gz', Z),
         ('rk', Z * Z), ('rv', Z * Z), ('sk', Z * Z), ('sv', Z * Z), ('fk', Z), ('fv', Z))
N_SEM = sum(n for _, n in KINDS)


def dot(a, b, ca, cb):
    return lax.dot_general(a, b, (((ca,), (cb,)), ((), ())), preferred_element_type=f32)


def tile(n):
    return slice(n * T, (n + 1) * T)


def rem(n, k=Z):
    return n % k if isinstance(n, int) else lax.rem(n, jnp.int32(k))


def div(n, k=Z):
    return n // k if isinstance(n, int) else lax.div(n, jnp.int32(k))


def sub_rows(n):
    return pl.ds(pl.multiple_of(SUB * n, SUB), SUB)


def body(q_hbm, k_hbm, v_hbm, do_hbm, o_out, dq_out, dk_out, dv_out,
         k_loc, v_loc, q_all, do_all, k_all, v_all, kt, vt, ot, dqt, dk, dv, cache, scb, dpb, mx_run,
         m_run, l_run, st_loc, st_par, st_col, ld,
         or1, or2, dqr1, dqr2, dkr1, dvr1, dk2, dv2, dkr2, dvr2, kst, vst, dk_fin, dv_fin, s_sem, r_sem):
    a = lax.axis_index('ctxo')
    b = lax.axis_index('ctx')
    z = div(b, Z * Z)
    y = rem(div(b))
    x = rem(b)
    m_blk = Z * y + x
    i_own = Z * a + z
    pa = 1 - a
    par = rem(a + z, 2)
    base = {}
    for kind, n in KINDS:
        base[kind] = sum(base[p][1] for p in base), n

    def dev(a_, z_, y_, x_):
        return {'ctxo': a_, 'ctx': Z * Z * z_ + Z * y_ + x_}

    partner = dev(pa, z, y, x)

    def col(d):
        return dev(a, rem(z + d), y, x)

    def other_col(d):
        return dev(pa, rem(z + d), y, x)

    def in_y(d):
        return dev(a, z, rem(y + d), x)

    def in_x(d):
        return dev(a, z, y, rem(x + d))

    def rc(kind, n_s, n_r, src, dst, to):
        off = base[kind][0]
        return pltpu.make_async_remote_copy(src_ref=src, dst_ref=dst, send_sem=s_sem.at[off + n_s], recv_sem=r_sem.at[off + n_r],
                                            device_id=to, device_id_type=MESH)

    def send(kind, n_s, n_r, src, dst, to):
        rc(kind, n_s, n_r, src, dst, to).start()

    def got(kind, n, ref):
        rc(kind, n, n, ref, ref, partner).wait_recv()

    def sent(kind, n, ref):
        rc(kind, n, n, ref, ref, partner).wait_send()

    def when(cond, fn, *args):
        pl.when(cond)(functools.partial(fn, *args))

    def group_of(s):
        a_s = div(s, 2)
        return a_s, 2 * rem(s, 2) + rem(a_s + a, 2)

    def g_of(s):
        a_s, z_s = group_of(s)
        return Z * a_s + z_s

    def not_mine(s):
        return g_of(s) != i_own

    own = [(q_hbm, q_all.at[i_own]), (do_hbm, do_all.at[i_own]), (k_hbm, k_loc), (v_hbm, v_loc)]
    own = [pltpu.make_async_copy(src, dst, s_sem.at[base['in'][0] + n]) for n, (src, dst) in enumerate(own)]
    for c in reversed(own):
        c.start()
    bar = pltpu.get_barrier_semaphore()
    peers = [partner] + [f(d) for d in OFFS for f in (col, other_col, in_y, in_x)]
    for to in peers:
        pl.semaphore_signal(bar, inc=1, device_id=to, device_id_type=MESH)
    for c in reversed(own):
        c.wait()
    pl.semaphore_wait(bar, len(peers))

    k5 = k_all.reshape(Z, Z, Z, SUB, HD)
    v5 = v_all.reshape(Z, Z, Z, SUB, HD)

    s_me = 2 * a + div(z, 2)
    keep = par == a
    for d in QUAD:
        rows = sub_rows(rem(z + d))
        to = dev(par, rem(z + d), y, x)

        def give():
            send('ka', d, s_me, k_loc.at[rows], k5.at[s_me, y, x], to)
            send('va', d, s_me, v_loc.at[rows], v5.at[s_me, y, x], to)

        if d:
            give()
        else:
            @pl.when(keep)
            def _():
                k_all[s_me, sub_rows(m_blk), :] = k_loc[rows, :]
                v_all[s_me, sub_rows(m_blk), :] = v_loc[rows, :]
            when(jnp.logical_not(keep), give)
    send('q', i_own, i_own, q_all.at[i_own], q_all.at[i_own], partner)
    send('do', i_own, i_own, do_all.at[i_own], do_all.at[i_own], partner)
    dk[...] = jnp.zeros(dk.shape, f32)
    dv[...] = jnp.zeros(dv.shape, f32)

    def kv_share():
        for s in QUAD:
            @pl.when(not_mine(s))
            def _():
                got('ka', s, k5.at[s, y, x])
                got('va', s, v5.at[s, y, x])
        for d in OFFS:
            send('kx', d, d, k5.at[:, y, x], k5.at[:, y, x], in_x(d))
            send('vy', d, d, v5.at[:, y, x], v5.at[:, y, x], in_y(d))

    def kv_spread():
        for d in OFFS:
            got('kx', d, k5.at[:, y, rem(x + Z - d)])
            got('vy', d, v5.at[:, rem(y + Z - d), x])
        for s in QUAD:
            for d in OFFS:
                n = Z * s + d
                send('ky', n, n, k5.at[s, y], k5.at[s, y], in_y(d))
                send('vx', n, n, v5.at[s, :, x], v5.at[s, :, x], in_x(d))

    def kv_ready(s):
        for d in OFFS:
            got('ky', Z * s + d, k5.at[s, rem(y + Z - d)])
            got('vx', Z * s + d, v5.at[s, :, rem(x + Z - d)])
        kt[s] = k_all[s].T
        vt[s] = v_all[s].T

    def half(ref, h):
        return ref.at[pl.ds(h * HALF, HALF)]

    def near_send(kind, full):
        for d in NEAR:
            send(kind, rem(i_own + d, G), i_own, full.at[i_own], full.at[i_own], col(d))

    def pass_on(kind, full, i_r, n):
        send(kind + 'f', n, rem(i_r), full.at[i_r], full.at[i_r], partner)

    def near_got(kind, full):
        for h, d in enumerate(NEAR):
            i_r = Z * a + rem(z + Z - d)
            got(kind, i_r, full.at[i_r])
            pass_on(kind, full, i_r, d)
            send(kind + 'h', h, h, half(full.at[i_r], h), half(full.at[i_r], h), col(d))

    def far_got(kind, full):
        i_r = Z * a + rem(z + 2)
        for h in range(2):
            got(kind + 'h', h, half(full.at[i_r], h))
        pass_on(kind, full, i_r, 2)

    def passed(kind, full, d):
        i_r = Z * pa + rem(z + Z - d)
        if d:
            got(kind + 'f', rem(i_r), full.at[i_r])
        else:
            got(kind, i_r, full.at[i_r])

    kv_share()
    when(a == 1, near_send, 'q', q_all)
    dqt[...] = jnp.zeros(dqt.shape, f32)
    ot[...] = jnp.zeros(ot.shape, f32)
    m_run[...] = jnp.full(m_run.shape, NEG, f32)
    l_run[...] = jnp.zeros(l_run.shape, f32)
    kv_spread()

    @pl.when(a == 1)
    def _():
        near_got('q', q_all)
        near_send('do', do_all)
    when(a == 0, near_send, 'q', q_all)

    def full_count(i):
        n = jnp.int32(0)
        for s in QUAD:
            n = n + (g_of(s) < i).astype(i32)
        return n

    def cache_at(i, s):
        n = i - g_of(s) - 1
        for r in OFFS:
            n = n + (r <= s) * (LAST - g_of(r - 1))
        return n

    def seen(j, ct):
        key_id = j * T + lax.broadcasted_iota(i32, (T, T), 0)
        pos = (ct * T + lax.broadcasted_iota(i32, (1, T), 1)) // Z
        last = SUB * m_blk + jnp.clip(pos - SUB * z, -1, SUB - 1)
        return key_id <= last

    def fold(p):
        return p.reshape(p.shape[0] // 8, 8, p.shape[1])

    def fwd_scores(i, s, pc, ct, j, mx, masked=False):
        t = dot(k_all[s, tile(j), :], q_all[i, tile(ct), :], 1, 1) * SCALE2
        if masked:
            t = jnp.where(seen(j, ct), t, -jnp.inf)
        cache[pc, tile(j), tile(ct)] = t
        r = jnp.max(fold(t), axis=0)
        return r if mx is None else jnp.maximum(mx, r)

    def fwd_first(i, s, pc, masked=False):
        mx = None
        for j in TILES:
            mx = fwd_scores(i, s, pc, 0, j, mx, masked)
        return mx

    def fwd_pair(i, s, pc, mx, i_n, pc_n, masked=False):
        for ct in TILES:
            cs = tile(ct)
            last = ct == NT - 1
            nxt = (i_n, s, pc_n, 0) if last else (i, s, pc, ct + 1)
            m_old = m_run[i, :, cs]
            m_new = jnp.maximum(m_old, jnp.max(mx, axis=0, keepdims=True))
            al = jnp.exp2(m_old - m_new)
            mx = None
            lp = None
            o = None
            for j in TILES:
                mx = fwd_scores(*nxt, j, mx, masked and not last)
                p = jnp.exp2(cache[pc, tile(j), cs] - m_new)
                r = jnp.sum(fold(p), axis=0)
                lp = r if lp is None else lp + r
                oj = dot(vt[s, :, tile(j)], p.astype(bf16), 1, 0)
                o = oj if o is None else o + oj
            l_run[i, :, cs] = l_run[i, :, cs] * al + jnp.sum(lp, axis=0, keepdims=True)
            ot[i, :, cs] = ot[i, :, cs] * al + o
            m_run[i, :, cs] = m_new
        return mx

    def spread(lo, k):
        return lo + rem(z + k + (k >= 2) * (5 - 2 * k))

    def fwd_seg(e):
        s = rem(e)
        g = g_of(s)
        hi = jnp.where(e < Z, G, Z)

        def plain():
            @pl.when(e == 0)
            def _():
                @pl.when(a == 0)
                def _():
                    passed('q', q_all, 0)
                    for d in NEAR:
                        passed('q', q_all, d)

            def pair(k, mx):
                when((e == 0) & (k == 1) & (a == 1), far_got, 'q', q_all)
                when((e == 0) & (k == 2) & (a == 0), passed, 'q', q_all, 2)
                i = spread(Z, k)
                i_n = spread(Z, jnp.minimum(k + 1, Z - 1))
                return fwd_pair(i, s, cache_at(i, s), mx, i_n, cache_at(i_n, s))
            lax.fori_loop(0, Z, pair, fwd_first(spread(Z, 0), s, cache_at(spread(Z, 0), s)))

        def diagonal():
            i1 = jnp.minimum(g + 1, hi - 1)
            pc1 = jnp.where(g + 1 < hi, cache_at(i1, s), N_FULL)
            mx = fwd_pair(g, s, N_FULL, fwd_first(g, s, N_FULL, True), i1, pc1, True)

            def pair(i, mx):
                i_n = jnp.minimum(i + 1, hi - 1)
                return fwd_pair(i, s, cache_at(i, s), mx, i_n, cache_at(i_n, s))
            lax.fori_loop(g + 1, hi, pair, mx)
        when(e < Z, kv_ready, s)
        when(e < 2, plain)
        when(e >= 2, diagonal)

    def put(ref, at, *rows):
        for n, r in enumerate(rows):
            ref[(*at, slice(n, n + 1), slice(None))] = r

    def get(ref, *at):
        return [ref[(*at, slice(n, n + 1), slice(None))] for n in range(ref.shape[-2])]

    def fwd_done(i, c):
        z_i = rem(i)
        d_part = jnp.sum(do_all[i].T.astype(f32) * ot[i], axis=0, keepdims=True)
        put(st_loc, (i,), m_run[i], l_run[i], d_part)

        @pl.when(div(i) != a)
        def _():
            send('st', z_i, z_i, st_loc.at[i], st_par.at[z_i], partner)
        return c

    def out_give():
        for n in QUAD:
            send('o', n, n, ot.at[Z * pa + n], or1.at[n], partner)

    def pair_done(z_o):
        i = Z * a + z_o
        got('st', z_o, st_par.at[z_o])
        mine = get(st_loc, i)
        other = get(st_par, z_o)
        top = jnp.maximum(mine[0], other[0])
        w0 = jnp.exp2(mine[0] - top)
        w1 = jnp.exp2(other[0] - top)
        put(st_col, (z_o, z), top, *[w0 * p + w1 * q for p, q in zip(mine[1:], other[1:])])
        for d in OFFS:
            send('sz', Z * z_o + d, Z * z_o + d, st_col.at[z_o, z], st_col.at[z_o, z], col(d))

    def out_join(z_o):
        i = Z * a + z_o
        got('o', z_o, or1.at[z_o])
        top = get(st_col, z_o, z)[0]
        w0 = jnp.exp2(get(st_loc, i)[0] - top)
        w1 = jnp.exp2(get(st_par, z_o)[0] - top)
        for ct in TILES:
            cs = tile(ct)
            ot[i, :, cs] = ot[i, :, cs] * w0[:, cs] + or1[z_o, :, cs] * w1[:, cs]
        h = rem(z_o + Z - z)

        @pl.when(h != 0)
        def _():
            send('oz', z_o, h, ot.at[i], or2.at[h - 1], dev(a, z_o, y, x))

    def col_done(z_o):
        i = Z * a + z_o
        for d in OFFS:
            got('sz', Z * z_o + d, st_col.at[z_o, rem(z + Z - d)])
        parts = [get(st_col, z_o, n) for n in QUAD]
        big = functools.reduce(jnp.maximum, [p[0] for p in parts])
        w = [jnp.exp2(p[0] - big) for p in parts]
        tot = sum(wn * p[1] for wn, p in zip(w, parts))
        dsum = sum(wn * p[2] for wn, p in zip(w, parts))
        put(ld, (i,), big + jnp.log(tot) * math.log2(math.e), dsum / tot)
        send('ld', i, i, ld.at[i], ld.at[i], partner)

    def passed_all(kind, full):
        for d in (0,) + OFFS:
            passed(kind, full, d)

    def seg_step(e, c):
        fwd_seg(e)

        @pl.when(a == 1)
        def _():
            when(e == 0, near_got, 'do', do_all)
            when(e == 1, far_got, 'do', do_all)

            @pl.when(e == 1)
            def _():
                for d in (0,) + NEAR:
                    passed('q', q_all, d)

            @pl.when(e == 3)
            def _():
                passed('q', q_all, 2)
                lax.fori_loop(Z, G, fwd_done, 0)
                for n in (3, 2, 1, 0):
                    pair_done(n)

            @pl.when(e == 4)
            def _():
                for n in (3, 2, 1, 0):
                    col_done(n)

            @pl.when(e == 5)
            def _():
                passed_all('do', do_all)
                lax.fori_loop(0, Z, fwd_done, 0)
                out_give()
                for d in (2, 1, 3, 0):
                    out_join(rem(z + d))

        @pl.when(a == 0)
        def _():
            @pl.when(e == 0)
            def _():
                near_got('q', q_all)
                near_send('do', do_all)
            when(e == 1, far_got, 'q', q_all)
            when(e == 2, near_got, 'do', do_all)

            @pl.when(e == 3)
            def _():
                passed_all('do', do_all)
                lax.fori_loop(Z, G, fwd_done, 0)
                out_give()
                far_got('do', do_all)

            @pl.when(e == 5)
            def _():
                lax.fori_loop(0, Z, fwd_done, 0)
        return c
    lax.fori_loop(0, 6, seg_step, 0)

    def dq_join(z_o):
        i = Z * a + z_o
        got('g', z_o, dqr1.at[z_o])
        for ct in TILES:
            cs = tile(ct)
            dqt[i, :, cs] = dqt[i, :, cs] + dqr1[z_o, :, cs]
        h = rem(z_o + Z - z)

        @pl.when(h != 0)
        def _():
            send('gz', z_o, h, dqt.at[i], dqr2.at[h - 1], dev(a, z_o, y, x))

    def bwd_scores(i, s, u, masked):
        j, ct = divmod(u, NT)
        dpb[u % NT] = dot(v_all[s, tile(j), :], do_all[i, tile(ct), :], 1, 1)
        if masked:
            t = dot(k_all[s, tile(j), :], q_all[i, tile(ct), :], 1, 1) * SCALE2
            scb[u % NT] = jnp.where(seen(j, ct), t, -jnp.inf)

    def bwd_pair(i, s, pc, s_n, masked=False):
        acc_v = None
        acc_k = None
        pend = None

        def products(u, p, ds, acc_v, acc_k):
            j, ct = divmod(u, NT)
            e = dot(p, do_all[i, tile(ct), :], 1, 0)
            g = dot(ds, q_all[i, tile(ct), :], 1, 0)
            acc_v = e if ct == 0 else acc_v + e
            acc_k = g if ct == 0 else acc_k + g
            dqt[i, :, tile(ct)] += dot(kt[s, :, tile(j)], ds, 1, 0)
            if ct == NT - 1:
                dv[s, tile(j), :] += acc_v
                dk[s, tile(j), :] += acc_k
            return acc_v, acc_k

        n_u = NT * NT
        for u in range(n_u):
            j, ct = divmod(u, NT)
            if u < n_u - 1:
                bwd_scores(i, s, u + 1, masked)
            else:
                bwd_scores(i, s_n, 0, False)
            t = scb[u % NT] if masked else cache[pc, tile(j), tile(ct)]
            p = jnp.exp2(t - ld[i, 0:1, tile(ct)])
            ds = p * (dpb[u % NT] - ld[i, 1:2, tile(ct)])
            now = p.astype(bf16), ds.astype(bf16)
            if pend is not None:
                acc_v, acc_k = products(u - 1, *pend, acc_v, acc_k)
            pend = now
        products(n_u - 1, *pend, acc_v, acc_k)

    def bwd_block(i, lo, hi):
        end = jnp.minimum(full_count(i), hi)
        s_d = 2 * div(i) + div(rem(i), 2)
        diag = (rem(div(i) + i, 2) == a) & (s_d >= lo) & (s_d < hi)

        @pl.when(diag)
        def _():
            bwd_scores(i, s_d, 0, True)
            bwd_pair(i, s_d, N_FULL, lo, True)

        @pl.when(jnp.logical_not(diag) & (lo < end))
        def _():
            bwd_scores(i, lo, 0, False)

        def pair(s, c):
            bwd_pair(i, s, cache_at(i, s), jnp.minimum(s + 1, Z - 1))
            return c
        lax.fori_loop(lo, end, pair, 0)

    dk5 = dk.reshape(Z, Z, Z, SUB, HD)
    dv5 = dv.reshape(Z, Z, Z, SUB, HD)
    dkr14 = dkr1.reshape(Z, 3, Z, SUB, HD)
    dvr14 = dvr1.reshape(Z, 3, Z, SUB, HD)
    dk24 = dk2.reshape(Z, Z, SUB, HD)
    dv24 = dv2.reshape(Z, Z, SUB, HD)

    def kv_first(s):
        for d in OFFS:
            n = Z * s + d
            send('rk', n, n, dk5.at[s, rem(y + d)], dkr14.at[s, d - 1], in_y(d))
            send('rv', n, n, dv5.at[s, :, rem(x + d)], dvr14.at[s, d - 1], in_x(d))

    def kv_second(s):
        for d in OFFS:
            got('rk', Z * s + d, dkr14.at[s, d - 1])
            got('rv', Z * s + d, dvr14.at[s, d - 1])
        dk2[s] = dk[s, pl.ds(pl.multiple_of(BLK * y, BLK), BLK), :] + sum(dkr1[s, d - 1] for d in OFFS)
        for n in QUAD:
            rows = slice(n * SUB, (n + 1) * SUB)
            dv2[s, rows, :] = dv[s, sub_rows(Z * n + x), :] + sum(dvr1[s, d - 1, rows, :] for d in OFFS)
        for d in OFFS:
            n = Z * s + d
            send('sk', n, n, dk24.at[s, rem(x + d)], dkr2.at[s, d - 1], in_x(d))
            send('sv', n, n, dv24.at[s, rem(y + d)], dvr2.at[s, d - 1], in_y(d))

    def kv_third(s):
        for d in OFFS:
            got('sk', Z * s + d, dkr2.at[s, d - 1])
            got('sv', Z * s + d, dvr2.at[s, d - 1])
        kst[s] = ((dk2[s, sub_rows(x), :] + sum(dkr2[s, d - 1] for d in OFFS)) * SCALE).astype(bf16)
        vst[s] = (dv2[s, sub_rows(y), :] + sum(dvr2[s, d - 1] for d in OFFS)).astype(bf16)
        a_s, z_s = group_of(s)
        rows = sub_rows(z)

        @pl.when(g_of(s) == i_own)
        def _():
            dk_fin[rows, :] = kst[s]
            dv_fin[rows, :] = vst[s]

        @pl.when(not_mine(s))
        def _():
            to = dev(a_s, z_s, y, x)
            send('fk', s, rem(z_s + Z - z), kst.at[s], dk_fin.at[rows], to)
            send('fv', s, rem(z_s + Z - z), vst.at[s], dv_fin.at[rows], to)

    def rot(k):
        return rem(z + 2 + Z - k + 3 * (k == 2) + (k == 3))

    def bwd_step(n, c):
        mid = (n == 4) | (n == 5)
        late = n >= 6
        i = jnp.where(mid, n - 2, jnp.where(late, rot(n - 6), LAST - n))
        lo = mid.astype(i32)
        hi = jnp.where(mid, 2, jnp.where(late, 1, Z))
        a_i = div(i)
        z_i = rem(i)
        when((a_i != a) & ((n < 6) | (z_i < 2)), got, 'ld', i, ld.at[i])
        bwd_block(i, lo, hi)

        @pl.when((a_i != a) & jnp.logical_not(mid))
        def _():
            send('g', z_i, z_i, dqt.at[i], dqr1.at[z_i], partner)
        for s in QUAD:
            when(n == (9, 5, 2, 0)[s] + a * (0, 0, 1, 1)[s], kv_first, s)

        @pl.when(a == 0)
        def _():
            @pl.when(n == 0)
            def _():
                for k in (2, 3, 1, 0):
                    pair_done(k)
                for d in (2, 1, 3, 0):
                    out_join(rem(z + d))

            @pl.when(n == 2)
            def _():
                for k in (2, 3, 1, 0):
                    col_done(k)
            when(n >= 7, dq_join, rot(n - 7))
        when((a == 1) & (n >= 1) & (n <= 4), dq_join, 4 - n)
        when(n == 2 + a, kv_second, 3)
        when(n == 5 + 2 * a, kv_second, 2)
        when(n == 6, kv_third, 3)
        when(n == 9, kv_third, 2)
        return c
    lax.fori_loop(0, 10, bwd_step, 0)

    when(a == 0, dq_join, z)
    kv_second(1)
    for h in OFFS:
        got('oz', h, or2.at[h - 1])
    w_z = [jnp.exp2(get(st_col, z, rem(z + Z - h))[0] - ld[i_own, 0:1, :]) for h in QUAD]
    for ct in TILES:
        cs = tile(ct)
        o = ot[i_own, :, cs] * w_z[0][:, cs]
        for h in OFFS:
            o = o + or2[h - 1, :, cs] * w_z[h][:, cs]
        o_out[cs, :] = o.T.astype(bf16)
    kv_second(0)
    kv_third(1)
    kv_third(0)
    for h in OFFS:
        got('gz', h, dqr2.at[h - 1])
    for ct in TILES:
        cs = tile(ct)
        dq_out[cs, :] = ((dqt[i_own, :, cs] + sum(dqr2[h - 1, :, cs] for h in OFFS)).T * SCALE).astype(bf16)
    for h in QUAD:
        rows = sub_rows(rem(z + Z - h))

        def take():
            got('fk', h, dk_fin.at[rows])
            got('fv', h, dv_fin.at[rows])
        if h:
            take()
        else:
            when(jnp.logical_not(keep), take)
    dk_out[...] = dk_fin[...]
    dv_out[...] = dv_fin[...]

    def left(n):
        sent('ka', n, k_loc.at[pl.ds(0, SUB)])
        sent('va', n, v_loc.at[pl.ds(0, SUB)])
    when(jnp.logical_not(keep), left, 0)
    for kind, full in (('q', q_all), ('do', do_all)):
        sent(kind, i_own, full.at[i_own])
        for h, d in enumerate(NEAR):
            sent(kind, rem(i_own + d, G), full.at[i_own])
            sent(kind + 'h', h, half(full.at[i_own], h))
        for d in OFFS:
            sent(kind + 'f', d, full.at[i_own])
    for d in OFFS:
        left(d)
        sent('kx', d, k5.at[:, y, x])
        sent('vy', d, v5.at[:, y, x])
    for s in QUAD:
        sent('st', s, st_par.at[s])
        sent('o', s, or1.at[s])
        sent('g', s, or1.at[s])
        sent('ld', Z * a + s, ld.at[s])

        @pl.when(s != z)
        def _():
            sent('oz', s, or1.at[s])
            sent('gz', s, or1.at[s])

        @pl.when(not_mine(s))
        def _():
            sent('fk', s, kst.at[s])
            sent('fv', s, vst.at[s])
        for d in OFFS:
            n = Z * s + d
            sent('sz', n, st_col.at[s, 0])
            sent('ky', n, k5.at[s, y])
            sent('vx', n, v5.at[s, :, x])
            sent('rk', n, dkr14.at[s, 0])
            sent('rv', n, dvr14.at[s, 0])
            sent('sk', n, dkr2.at[s, 0])
            sent('sv', n, dvr2.at[s, 0])


def solution(mesh):
    blk_spec = P('data', CTX_AXES, None, None)
    v = pltpu.VMEM
    big = (ROWS, HD)
    big_t = (HD, ROWS)
    blk = (BLK, HD)
    sub = (SUB, HD)
    scratch = [
        *[v(blk, bf16)] * 2,
        *[v((G,) + big, bf16)] * 2, *[v((Z,) + big, bf16)] * 2,
        *[v((Z,) + big_t, bf16)] * 2,
        *[v((G,) + big_t, f32)] * 2, *[v((Z,) + big, f32)] * 2,
        v((N_FULL + 1, ROWS, ROWS), f32),
        *[v((NT, T, T), f32)] * 2, v((8, T), f32),
        *[v((G, 1, ROWS), f32)] * 2, v((G, 3, ROWS), f32),
        v((Z, 3, ROWS), f32), v((Z, Z, 3, ROWS), f32), v((G, 2, ROWS), f32),
        *[v((Z,) + big_t, f32), v((3,) + big_t, f32)] * 2,
        *[v((Z, 3) + blk, f32)] * 2, *[v((Z,) + blk, f32)] * 2,
        *[v((Z, 3) + sub, f32)] * 2, *[v((Z,) + sub, bf16)] * 2,
        *[v(blk, bf16)] * 2,
        *[pltpu.SemaphoreType.DMA((N_SEM,))] * 2,
    ]
    call = pl.pallas_call(
        body,
        name='attn',
        out_shape=[jax.ShapeDtypeStruct(big, bf16)] * 2 + [jax.ShapeDtypeStruct(blk, bf16)] * 2,
        in_specs=[pl.BlockSpec(memory_space=pl.ANY)] * 4,
        out_specs=[pl.BlockSpec(memory_space=pltpu.VMEM)] * 4,
        scratch_shapes=scratch,
        compiler_params=pltpu.CompilerParams(collective_id=0, has_side_effects=True, vmem_limit_bytes=67043328),
    )

    def hand_out(*refs):
        for src, dst in zip(refs[:Z], refs[Z:]):
            dst[...] = src[...]

    leave = pl.pallas_call(
        hand_out,
        name='leave',
        out_shape=[jax.ShapeDtypeStruct(big, bf16)] * 2 + [jax.ShapeDtypeStruct(blk, bf16)] * 2,
        in_specs=[pl.BlockSpec(memory_space=pltpu.VMEM)] * 4,
        out_specs=[pl.BlockSpec(memory_space=pltpu.VMEM)] * 4,
    )

    def local_attn(q_in, k_in, v_in, do_in):
        o, dq, dk, dv = leave(*call(q_in.reshape(big), k_in.reshape(blk), v_in.reshape(blk), do_in.reshape(big)))
        return o.reshape(q_in.shape), dq.reshape(q_in.shape), dk.reshape(k_in.shape), dv.reshape(k_in.shape)

    return jax.shard_map(local_attn, mesh=mesh, in_specs=(blk_spec,) * 4, out_specs=(blk_spec,) * 4, check_vma=False)
```

```python
import functools
import math
import jax
import jax.numpy as jnp
from jax import lax
from jax.experimental import pallas as pl
from jax.experimental.pallas import tpu as pltpu
from jax.sharding import PartitionSpec as P

CTX_AXES = ('ctxo', 'ctx')
MESH = pl.DeviceIdType.MESH
f32 = jnp.float32
bf16 = jnp.bfloat16
i32 = jnp.int32

Z = 4
G = 8
HD = 128
SUB = 48
BLK = Z * SUB
ROWS = Z * BLK
HALF = ROWS // 2
T = 256
NT = ROWS // T
TILES = range(NT)
QUAD = range(Z)
OFFS = (1, 2, 3)
NEAR = (1, 3)
SCALE = 1.0 / math.sqrt(HD)
SCALE2 = SCALE * math.log2(math.e)
NEG = -1e30
N_PAIR = 18
LAST = G - 1

KINDS = {'ka': Z, 'va': Z, 'kx': 1, 'vy': 1, 'ky': Z, 'vx': Z,
         'q': 3, 'qh': 2, 'qf': Z, 'do': 3, 'doh': 2, 'dof': Z,
         'st': Z, 'sz': Z, 'ld': Z, 'o': Z, 'oz': 1, 'g': Z, 'gz': 1,
         'rk': Z, 'rv': Z, 'sk': Z, 'sv': Z, 'fk': 2, 'fv': 2}
N_RECV = sum(KINDS.values())
N_SEND = len(KINDS) + 2 * Z


def dot(a, b, ca, cb):
    return lax.dot_general(a, b, (((ca,), (cb,)), ((), ())), preferred_element_type=f32)


def tile(n):
    return slice(n * T, (n + 1) * T)


def rem(n, k=Z):
    return n % k if isinstance(n, int) else lax.rem(n, jnp.int32(k))


def div(n, k=Z):
    return n // k if isinstance(n, int) else lax.div(n, jnp.int32(k))


def sub_rows(n):
    return pl.ds(pl.multiple_of(SUB * n, SUB), SUB)


def body(q_hbm, k_hbm, v_hbm, do_hbm, o_hbm, dq_hbm, dk_hbm, dv_hbm,
         k_loc, v_loc, q_all, do_all, k_all, v_all, kt, vt, acc, dk, dv, cache, dpb,
         m_run, l_run, st_loc, st_par, st_col, ld,
         or1, or2, dqr2, dkr1, dvr1, dkr2, dvr2, kst, vst, dk_fin, dv_fin, s_sem, r_sem, room):
    a = lax.axis_index('ctxo')
    b = lax.axis_index('ctx')
    z = div(b, Z * Z)
    y = rem(div(b))
    x = rem(b)
    m_blk = Z * y + x
    i_own = Z * a + z
    pa = 1 - a
    par = rem(a + z, 2)
    names = list(KINDS)
    base = {kind: sum(KINDS[k] for k in names[:n]) for n, kind in enumerate(names)}

    def dev(a_, z_, y_, x_):
        return {'ctxo': a_, 'ctx': Z * Z * z_ + Z * y_ + x_}

    partner = dev(pa, z, y, x)

    def col(d):
        return dev(a, rem(z + d), y, x)

    def other_col(d):
        return dev(pa, rem(z + d), y, x)

    def in_y(d):
        return dev(a, z, rem(y + d), x)

    def in_x(d):
        return dev(a, z, y, rem(x + d))

    def rc(kind, n, src, dst, to):
        return pltpu.make_async_remote_copy(src_ref=src, dst_ref=dst, send_sem=s_sem.at[names.index(kind)], recv_sem=r_sem.at[base[kind] + n],
                                            device_id=to, device_id_type=MESH)

    def send(kind, n, src, dst, to):
        rc(kind, n, src, dst, to).start()

    def got(kind, n, ref):
        rc(kind, n, ref, ref, partner).wait_recv()

    def sent(kind, ref):
        rc(kind, 0, ref, ref, partner).wait_send()

    def when(cond, fn, *args):
        pl.when(cond)(functools.partial(fn, *args))

    def group_of(s):
        a_s = div(s, 2)
        return a_s, 2 * rem(s, 2) + rem(a_s + a, 2)

    def g_of(s):
        a_s, z_s = group_of(s)
        return Z * a_s + z_s

    def not_mine(s):
        return g_of(s) != i_own

    own = [(q_hbm, q_all.at[i_own]), (do_hbm, do_all.at[i_own]), (k_hbm, k_loc), (v_hbm, v_loc)]
    own = [pltpu.make_async_copy(src, dst, s_sem.at[len(KINDS) + n]) for n, (src, dst) in enumerate(own)]
    for c in reversed(own):
        c.start()
    bar = pltpu.get_barrier_semaphore()
    peers = [partner] + [f(d) for d in OFFS for f in (col, other_col, in_y, in_x)]
    for to in peers:
        pl.semaphore_signal(bar, inc=1, device_id=to, device_id_type=MESH)
    for c in reversed(own):
        c.wait()
    pl.semaphore_wait(bar, len(peers))

    QUADS = pl.ds(0, Z)
    OTHERS = pl.ds(0, 3)
    k5 = k_all.reshape(Z, Z, Z, SUB, HD)
    v5 = v_all.reshape(Z, Z, Z, SUB, HD)

    s_me = 2 * a + div(z, 2)
    keep = par == a
    for d in QUAD:
        rows = sub_rows(rem(z + d))
        to = dev(par, rem(z + d), y, x)

        def give():
            send('ka', s_me, k_loc.at[rows], k5.at[s_me, y, x], to)
            send('va', s_me, v_loc.at[rows], v5.at[s_me, y, x], to)

        if d:
            give()
        else:
            @pl.when(keep)
            def _():
                k_all[s_me, sub_rows(m_blk), :] = k_loc[rows, :]
                v_all[s_me, sub_rows(m_blk), :] = v_loc[rows, :]
            when(jnp.logical_not(keep), give)
    send('q', 2, q_all.at[i_own], q_all.at[i_own], partner)
    send('do', 2, do_all.at[i_own], do_all.at[i_own], partner)
    dk[...] = jnp.zeros(dk.shape, f32)
    dv[...] = jnp.zeros(dv.shape, f32)

    def kv_share():
        for s in QUAD:
            @pl.when(not_mine(s))
            def _():
                got('ka', s, k5.at[s, y, x])
                got('va', s, v5.at[s, y, x])
        for d in OFFS:
            send('kx', 0, k5.at[:, y, x], k5.at[:, y, x], in_x(d))
            send('vy', 0, v5.at[:, y, x], v5.at[:, y, x], in_y(d))

    def kv_spread():
        got('kx', 0, k5.at[:, OTHERS, 0])
        got('vy', 0, v5.at[:, OTHERS, 0])
        for s in QUAD:
            for d in OFFS:
                send('ky', s, k5.at[s, y], k5.at[s, y], in_y(d))
                send('vx', s, v5.at[s, :, x], v5.at[s, :, x], in_x(d))

    def kv_ready(s):
        got('ky', s, k5.at[s, OTHERS])
        got('vx', s, v5.at[s, OTHERS])
        kt[s] = k_all[s].T
        vt[s] = v_all[s].T

    def half(ref, h):
        return ref.at[pl.ds(h * HALF, HALF)]

    def near_send(kind, full):
        for h, d in enumerate(NEAR):
            send(kind, h, full.at[i_own], full.at[i_own], col(d))

    def pass_on(kind, full, i_r, n):
        send(kind + 'f', n, full.at[i_r], full.at[i_r], partner)

    def near_got(kind, full):
        for h, d in enumerate(NEAR):
            i_r = Z * a + rem(z + Z - d)
            got(kind, h, full.at[i_r])
            pass_on(kind, full, i_r, d)
            send(kind + 'h', h, half(full.at[i_r], h), half(full.at[i_r], h), col(d))

    def far_got(kind, full):
        i_r = Z * a + rem(z + 2)
        for h in range(2):
            got(kind + 'h', h, half(full.at[i_r], h))
        pass_on(kind, full, i_r, 2)

    def passed(kind, full, d):
        i_r = Z * pa + rem(z + Z - d)
        if d:
            got(kind + 'f', d, full.at[i_r])
        else:
            got(kind, 2, full.at[i_r])

    kv_share()
    when(a == 1, near_send, 'q', q_all)
    acc[...] = jnp.zeros(acc.shape, f32)
    m_run[...] = jnp.full(m_run.shape, NEG, f32)
    l_run[...] = jnp.zeros(l_run.shape, f32)
    kv_spread()

    @pl.when(a == 1)
    def _():
        near_got('q', q_all)
        near_send('do', do_all)
    when(a == 0, near_send, 'q', q_all)

    def cache_at(i, s):
        n = i - g_of(s)
        for r in OFFS:
            n = n + (r <= s) * (G - g_of(r - 1))
        return n

    def dq_at(i):
        return jnp.where(div(i) == a, G + rem(i), i)

    def seen(j, ct):
        key_id = j * T + lax.broadcasted_iota(i32, (T, T), 0)
        pos = (ct * T + lax.broadcasted_iota(i32, (1, T), 1)) // Z
        last = SUB * m_blk + jnp.clip(pos - SUB * z, -1, SUB - 1)
        return key_id <= last

    def fold(p):
        return p.reshape(p.shape[0] // 8, 8, p.shape[1])

    def fwd_scores(i, s, pc, ct, j, mx, masked=False):
        t = dot(k_all[s, tile(j), :], q_all[i, tile(ct), :], 1, 1) * SCALE2
        if masked:
            t = jnp.where(seen(j, ct), t, -jnp.inf)
        cache[pc, tile(j), tile(ct)] = t
        r = jnp.max(fold(t), axis=0)
        return r if mx is None else jnp.maximum(mx, r)

    def fwd_first(i, s, masked=False):
        mx = None
        for j in TILES:
            mx = fwd_scores(i, s, cache_at(i, s), 0, j, mx, masked)
        return mx

    def fwd_pair(i, s, mx, i_n, s_n, pc, pc_n, masked=False):
        for ct in TILES:
            cs = tile(ct)
            last = ct == NT - 1
            nxt = (i_n, s_n, pc_n, 0) if last else (i, s, pc, ct + 1)
            m_old = m_run[i, :, cs]
            m_new = jnp.maximum(m_old, jnp.max(mx, axis=0, keepdims=True))
            al = jnp.exp2(m_old - m_new)
            mx = None
            lp = None
            o = None
            for j in TILES:
                mx = fwd_scores(*nxt, j, mx, masked and not last)
                p = jnp.exp2(cache[pc, tile(j), cs] - m_new)
                r = jnp.sum(fold(p), axis=0)
                lp = r if lp is None else lp + r
                oj = dot(vt[s, :, tile(j)], p.astype(bf16), 1, 0)
                o = oj if o is None else o + oj
            l_run[i, :, cs] = l_run[i, :, cs] * al + jnp.sum(lp, axis=0, keepdims=True)
            acc[i, :, cs] = acc[i, :, cs] * al + o
            m_run[i, :, cs] = m_new
        return mx

    def spread(lo, k):
        return lo + rem(z + k + (k >= 2) * (5 - 2 * k))

    def fwd_seg(e):
        s = rem(e)
        g = g_of(s)
        hi = jnp.where(e < Z, G, Z)
        at = cache_at(0, s)

        def plain():
            @pl.when(e == 0)
            def _():
                @pl.when(a == 0)
                def _():
                    passed('q', q_all, 0)
                    for d in NEAR:
                        passed('q', q_all, d)

            def pair(k, mx):
                when((e == 0) & (k == 1) & (a == 1), far_got, 'q', q_all)
                when((e == 0) & (k == 2) & (a == 0), passed, 'q', q_all, 2)
                i = spread(Z, k)
                i_n = spread(Z, jnp.minimum(k + 1, Z - 1))
                return fwd_pair(i, s, mx, i_n, s, at + i, at + i_n)
            lax.fori_loop(0, Z, pair, fwd_first(spread(Z, 0), s))

        def diagonal():
            more = g + 1 < hi
            mx = fwd_pair(g, s, fwd_first(g, s, True), jnp.where(more, g + 1, LAST), jnp.where(more, s, 0),
                          at + g, jnp.where(more, at + g + 1, cache_at(LAST, 0)), True)

            def pair(i, mx):
                i_n = jnp.minimum(i + 1, hi - 1)
                return fwd_pair(i, s, mx, i_n, s, at + i, at + i_n)
            lax.fori_loop(g + 1, hi, pair, mx)
        when(e < Z, kv_ready, s)
        when(e < 2, plain)
        when(e >= 2, diagonal)

    def put(ref, at, *rows):
        for n, r in enumerate(rows):
            ref[(*at, slice(n, n + 1), slice(None))] = r

    def get(ref, *at):
        return [ref[(*at, slice(n, n + 1), slice(None))] for n in range(ref.shape[-2])]

    def fwd_done(i, c):
        z_i = rem(i)
        d_part = jnp.sum(do_all[i].T.astype(f32) * acc[i], axis=0, keepdims=True)
        put(st_loc, (i,), m_run[i], l_run[i], d_part)

        @pl.when(div(i) != a)
        def _():
            send('st', z_i, st_loc.at[i], st_par.at[z_i], partner)
        return c

    def out_give():
        for n in QUAD:
            send('o', n, acc.at[Z * pa + n], or1.at[n], partner)

    def pair_done(z_o):
        i = Z * a + z_o
        got('st', z_o, st_par.at[z_o])
        mine = get(st_loc, i)
        other = get(st_par, z_o)
        top = jnp.maximum(mine[0], other[0])
        w0 = jnp.exp2(mine[0] - top)
        w1 = jnp.exp2(other[0] - top)
        put(st_col, (z_o, z), top, *[w0 * p + w1 * q for p, q in zip(mine[1:], other[1:])])
        for d in OFFS:
            send('sz', z_o, st_col.at[z_o, z], st_col.at[z_o, z], col(d))

    def out_join(z_o):
        i = Z * a + z_o
        got('o', z_o, or1.at[z_o])
        top = get(st_col, z_o, z)[0]
        w0 = jnp.exp2(get(st_loc, i)[0] - top)
        w1 = jnp.exp2(get(st_par, z_o)[0] - top)
        for ct in TILES:
            cs = tile(ct)
            acc[i, :, cs] = acc[i, :, cs] * w0[:, cs] + or1[z_o, :, cs] * w1[:, cs]
        h = rem(z_o + Z - z)

        @pl.when(h != 0)
        def _():
            send('oz', 0, acc.at[i], or2.at[h - 1], dev(a, z_o, y, x))

    def joins():
        for d in (2, 1, 3, 0):
            out_join(rem(z + d))
        pl.semaphore_signal(room, inc=1, device_id=partner, device_id_type=MESH)

    def col_done(z_o):
        i = Z * a + z_o
        got('sz', z_o, st_col.at[z_o, OTHERS])
        parts = [get(st_col, z_o, n) for n in QUAD]
        big = functools.reduce(jnp.maximum, [p[0] for p in parts])
        w = [jnp.exp2(p[0] - big) for p in parts]
        tot = sum(wn * p[1] for wn, p in zip(w, parts))
        dsum = sum(wn * p[2] for wn, p in zip(w, parts))
        put(ld, (i,), big + jnp.log(tot) * math.log2(math.e), dsum / tot)
        send('ld', z_o, ld.at[i], ld.at[i], partner)

    def passed_all(kind, full):
        for d in (0,) + OFFS:
            passed(kind, full, d)

    def seg_step(e, c):
        fwd_seg(e)

        @pl.when(a == 1)
        def _():
            when(e == 0, near_got, 'do', do_all)
            when(e == 1, far_got, 'do', do_all)

            @pl.when(e == 1)
            def _():
                for d in (0,) + NEAR:
                    passed('q', q_all, d)

            @pl.when(e == 3)
            def _():
                passed('q', q_all, 2)
                lax.fori_loop(Z, G, fwd_done, 0)
                for n in (3, 2, 1, 0):
                    pair_done(n)

            @pl.when(e == 4)
            def _():
                for n in (3, 2, 1, 0):
                    col_done(n)

            @pl.when(e == 5)
            def _():
                passed_all('do', do_all)
                lax.fori_loop(0, Z, fwd_done, 0)
                out_give()
                joins()

        @pl.when(a == 0)
        def _():
            @pl.when(e == 0)
            def _():
                near_got('q', q_all)
                near_send('do', do_all)
            when(e == 1, far_got, 'q', q_all)
            when(e == 2, near_got, 'do', do_all)

            @pl.when(e == 3)
            def _():
                passed_all('do', do_all)
                lax.fori_loop(Z, G, fwd_done, 0)
                out_give()
                far_got('do', do_all)

            @pl.when(e == 5)
            def _():
                lax.fori_loop(0, Z, fwd_done, 0)
        return c
    lax.fori_loop(0, 6, seg_step, 0)

    def dq_join(z_o):
        i = G + z_o
        got('g', z_o, or1.at[z_o])
        for ct in TILES:
            cs = tile(ct)
            acc[i, :, cs] = acc[i, :, cs] + or1[z_o, :, cs]
        h = rem(z_o + Z - z)

        @pl.when(h != 0)
        def _():
            send('gz', 0, acc.at[i], dqr2.at[h - 1], dev(a, z_o, y, x))

    def dq_room():
        sent('o', or1)
        for n in QUAD:
            acc[Z * pa + n] = jnp.zeros(or1.shape[1:], f32)

    def bwd_scores(i, s, u):
        j, ct = divmod(u, NT)
        dpb[u % NT] = dot(v_all[s, tile(j), :], do_all[i, tile(ct), :], 1, 1)

    def bwd_pair(i, s, i_n, s_n, pc, dq):
        acc_v = None
        acc_k = None
        pend = None

        def products(u, p, ds, acc_v, acc_k):
            j, ct = divmod(u, NT)
            e = dot(p, do_all[i, tile(ct), :], 1, 0)
            g = dot(ds, q_all[i, tile(ct), :], 1, 0)
            acc_v = e if ct == 0 else acc_v + e
            acc_k = g if ct == 0 else acc_k + g
            acc[dq, :, tile(ct)] += dot(kt[s, :, tile(j)], ds, 1, 0)
            if ct == NT - 1:
                dv[s, tile(j), :] += acc_v
                dk[s, tile(j), :] += acc_k
            return acc_v, acc_k

        n_u = NT * NT
        for u in range(n_u):
            j, ct = divmod(u, NT)
            if u < n_u - 1:
                bwd_scores(i, s, u + 1)
            else:
                bwd_scores(i_n, s_n, 0)
            p = jnp.exp2(cache[pc, tile(j), tile(ct)] - ld[i, 0:1, tile(ct)])
            ds = p * (dpb[u % NT] - ld[i, 1:2, tile(ct)])
            now = p.astype(bf16), ds.astype(bf16)
            if pend is not None:
                acc_v, acc_k = products(u - 1, *pend, acc_v, acc_k)
            pend = now
        products(n_u - 1, *pend, acc_v, acc_k)

    def rot(k):
        return rem(z + (2, 1, 3, 0)[k])

    STEPS = 10

    def bwd_part(n):
        i, lo, hi = (LAST - n, 0, Z) if n < 4 else (n - 2, 1, 2) if n < 6 else (rot(n - 6), 0, 1)
        end = jnp.int32(0)
        for s in QUAD:
            end = end + (g_of(s) <= i).astype(i32)
        return i, lo, jnp.minimum(end, hi)

    def bwd_block(n):
        i, lo, end = bwd_part(n)
        i_n, lo_n, _ = bwd_part(min(n + 1, STEPS - 1))
        _, lo_p, end_p = bwd_part(max(n - 1, 0))

        if n == 0:
            bwd_scores(i, lo, 0)
        elif n > 4:
            when((lo < end) & (lo_p >= end_p), bwd_scores, i, lo, 0)
        dq = dq_at(i)

        def pair(s, c):
            more = s + 1 < end
            bwd_pair(i, s, jnp.where(more, i, i_n), jnp.where(more, s + 1, lo_n), cache_at(i, s), dq)
            return c
        lax.fori_loop(lo, end, pair, 0)

    dk5 = dk.reshape(Z, Z, Z, SUB, HD)
    dv5 = dv.reshape(Z, Z, Z, SUB, HD)
    dkr14 = dkr1.reshape(Z, 3, Z, SUB, HD)
    dvr14 = dvr1.reshape(Z, 3, Z, SUB, HD)

    def kv_first(s):
        for d in OFFS:
            send('rk', s, dk5.at[s, rem(y + d)], dkr14.at[s, d - 1], in_y(d))
            send('rv', s, dv5.at[s, :, rem(x + d)], dvr14.at[s, d - 1], in_x(d))

    def kv_second(s):
        got('rk', s, dkr1.at[s])
        got('rv', s, dvr1.at[s])
        rows = pl.ds(pl.multiple_of(BLK * y, BLK), BLK)
        dk[s, rows, :] = dk[s, rows, :] + sum(dkr1[s, d - 1] for d in OFFS)
        for n in QUAD:
            rows = sub_rows(Z * n + x)
            dv[s, rows, :] = dv[s, rows, :] + sum(dvr1[s, d - 1, n * SUB:(n + 1) * SUB, :] for d in OFFS)
        for d in OFFS:
            send('sk', s, dk5.at[s, y, rem(x + d)], dkr2.at[s, d - 1], in_x(d))
            send('sv', s, dv5.at[s, rem(y + d), x], dvr2.at[s, d - 1], in_y(d))

    def kv_third(s):
        got('sk', s, dkr2.at[s])
        got('sv', s, dvr2.at[s])
        kst[s] = ((dk[s, sub_rows(m_blk), :] + sum(dkr2[s, d - 1] for d in OFFS)) * SCALE).astype(bf16)
        vst[s] = (dv[s, sub_rows(m_blk), :] + sum(dvr2[s, d - 1] for d in OFFS)).astype(bf16)
        a_s, z_s = group_of(s)
        rows = sub_rows(z)

        @pl.when(g_of(s) == i_own)
        def _():
            dk_fin[rows, :] = kst[s]
            dv_fin[rows, :] = vst[s]

        @pl.when(not_mine(s))
        def _():
            to = dev(a_s, z_s, y, x)
            far = (z_s != z).astype(i32)
            send('fk', far, kst.at[s], dk_fin.at[rows], to)
            send('fv', far, vst.at[s], dv_fin.at[rows], to)

    def bwd_step(n):
        i, lo, _ = bwd_part(n)
        a_i = div(i)
        z_i = rem(i)
        to = 0 if n < 4 else 1
        mine = a == to
        if n in (0, 2):
            when(a == n // 2, dq_room)
        when(mine if n < 6 else mine & (z_i < 2), got, 'ld', z_i, ld.at[i])
        bwd_block(n)

        def give():
            send('g', z_i, acc.at[i], or1.at[z_i], partner)
        if n in (0, 6):
            when(mine, pl.semaphore_wait, room, 1)
        if lo == 0:
            when(mine, give)
        for core, firsts, seconds, thirds, joined in (
                (0, {0: 3, 2: 2, 5: 1, 9: 0}, {2: 3, 5: 2}, {7: 3}, {7: rot(0), 8: rot(1), 9: rot(2)}),
                (1, {1: 3, 3: 2, 5: 1, 9: 0}, {3: 3, 7: 2}, {7: 3}, {1: 3, 2: 2, 3: 1, 5: 0})):
            def events():
                if n in firsts:
                    kv_first(firsts[n])
                if n == 0 and core == 0:
                    for k in (2, 3, 1, 0):
                        pair_done(k)
                    joins()
                if n == 2 and core == 0:
                    for k in (2, 3, 1, 0):
                        col_done(k)
                if n in joined:
                    dq_join(joined[n])
                if n in seconds:
                    kv_second(seconds[n])
                if n in thirds:
                    kv_third(thirds[n])
            when(a == core, events)

    for n in range(STEPS):
        bwd_step(n)

    when(a == 0, dq_join, z)
    kv_second(1)
    kv_third(2)
    sent('kx', k5.at[:, OTHERS, 0])
    sent('ky', k5.at[OTHERS])
    outs = [(k_all.at[0], o_hbm), (k_all.at[1], dq_hbm), (dk_fin, dk_hbm), (dv_fin, dv_hbm)]
    outs = [pltpu.make_async_copy(src, dst, s_sem.at[len(KINDS) + Z + n]) for n, (src, dst) in enumerate(outs)]
    got('oz', 0, or2)
    w_z = [jnp.exp2(get(st_col, z, rem(z + Z - h))[0] - ld[i_own, 0:1, :]) for h in QUAD]
    for ct in TILES:
        cs = tile(ct)
        o = acc[i_own, :, cs] * w_z[0][:, cs]
        for h in OFFS:
            o = o + or2[h - 1, :, cs] * w_z[h][:, cs]
        k_all[0, cs, :] = o.T.astype(bf16)
    outs[0].start()
    kv_second(0)
    kv_third(1)
    got('gz', 0, dqr2)
    for ct in TILES:
        cs = tile(ct)
        k_all[1, cs, :] = ((acc[G + z, :, cs] + sum(dqr2[h - 1, :, cs] for h in OFFS)).T * SCALE).astype(bf16)
    outs[1].start()
    kv_third(0)
    def take(n, rows):
        got('fk', n, dk_fin.at[rows])
        got('fv', n, dv_fin.at[rows])
    take(1, pl.ds(0, BLK - SUB))
    when(jnp.logical_not(keep), take, 0, pl.ds(0, SUB))
    outs[2].start()
    outs[3].start()

    def left(n):
        sent('ka', k_loc.at[pl.ds(0, n * SUB)])
        sent('va', v_loc.at[pl.ds(0, n * SUB)])
        sent('fk', kst.at[pl.ds(0, n)])
        sent('fv', vst.at[pl.ds(0, n)])
    when(keep, left, 3)
    when(jnp.logical_not(keep), left, Z)
    for kind, full in (('q', q_all), ('do', do_all)):
        sent(kind, full.at[OTHERS])
        sent(kind + 'h', full.at[0])
        sent(kind + 'f', full.at[OTHERS])
    for kind, ref in (('vy', v5.at[:, OTHERS, 0]), ('vx', v5.at[OTHERS]), ('st', st_par), ('g', or1), ('ld', ld.at[QUADS]), ('oz', or2), ('gz', dqr2),
                      ('sz', st_col.at[:, OTHERS]), ('rk', dkr1), ('rv', dvr1), ('sk', dkr2), ('sv', dvr2)):
        sent(kind, ref)
    for c in outs:
        c.wait()


def solution(mesh):
    blk_spec = P('data', CTX_AXES, None, None)
    v = pltpu.VMEM
    big = (ROWS, HD)
    big_t = (HD, ROWS)
    blk = (BLK, HD)
    sub = (SUB, HD)
    scratch = [
        *[v(blk, bf16)] * 2,
        *[v((G,) + big, bf16)] * 2, *[v((Z,) + big, bf16)] * 2,
        *[v((Z,) + big_t, bf16)] * 2,
        v((G + Z,) + big_t, f32), *[v((Z,) + big, f32)] * 2,
        v((N_PAIR, ROWS, ROWS), f32),
        v((NT, T, T), f32),
        *[v((G, 1, ROWS), f32)] * 2, v((G, 3, ROWS), f32),
        v((Z, 3, ROWS), f32), v((Z, Z, 3, ROWS), f32), v((G, 2, ROWS), f32),
        v((Z,) + big_t, f32), *[v((3,) + big_t, f32)] * 2,
        *[v((Z, 3) + blk, f32)] * 2,
        *[v((Z, 3) + sub, f32)] * 2, *[v((Z,) + sub, bf16)] * 2,
        *[v(blk, bf16)] * 2,
        pltpu.SemaphoreType.DMA((N_SEND,)), pltpu.SemaphoreType.DMA((N_RECV,)), pltpu.SemaphoreType.REGULAR,
    ]
    call = pl.pallas_call(
        body,
        name='attn',
        out_shape=[jax.ShapeDtypeStruct(big, bf16)] * 2 + [jax.ShapeDtypeStruct(blk, bf16)] * 2,
        in_specs=[pl.BlockSpec(memory_space=pl.ANY)] * 4,
        out_specs=[pl.BlockSpec(memory_space=pl.ANY)] * 4,
        scratch_shapes=scratch,
        compiler_params=pltpu.CompilerParams(collective_id=0, has_side_effects=True, vmem_limit_bytes=67043328),
    )

    def hand_out(*refs):
        srcs, dsts, bufs, sems = refs[:Z], refs[Z:2 * Z], refs[2 * Z:3 * Z], refs[3 * Z]
        ins = [pltpu.make_async_copy(src, buf, sems.at[0, n]) for n, (src, buf) in enumerate(zip(srcs, bufs))]
        outs = [pltpu.make_async_copy(buf, dst, sems.at[1, n]) for n, (buf, dst) in enumerate(zip(bufs, dsts))]
        for c in ins:
            c.start()
        for c, e in zip(ins, outs):
            c.wait()
            e.start()
        for e in outs:
            e.wait()

    leave = pl.pallas_call(
        hand_out,
        name='leave',
        out_shape=[jax.ShapeDtypeStruct(big, bf16)] * 2 + [jax.ShapeDtypeStruct(blk, bf16)] * 2,
        in_specs=[pl.BlockSpec(memory_space=pl.ANY)] * 4,
        out_specs=[pl.BlockSpec(memory_space=pl.ANY)] * 4,
        scratch_shapes=[*[v(big, bf16)] * 2, *[v(blk, bf16)] * 2, pltpu.SemaphoreType.DMA((2, Z))],
    )

    def local_attn(q_in, k_in, v_in, do_in):
        o, dq, dk, dv = leave(*call(q_in.reshape(big), k_in.reshape(blk), v_in.reshape(blk), do_in.reshape(big)))
        return o.reshape(q_in.shape), dq.reshape(q_in.shape), dk.reshape(k_in.shape), dv.reshape(k_in.shape)

    return jax.shard_map(local_attn, mesh=mesh, in_specs=(blk_spec,) * 4, out_specs=(blk_spec,) * 4, check_vma=False)
```

```python
import functools
import math
import jax
import jax.numpy as jnp
from jax import lax
from jax.experimental import pallas as pl
from jax.experimental.pallas import tpu as pltpu
from jax.sharding import PartitionSpec as P

CTX_AXES = ('ctxo', 'ctx')
MESH = pl.DeviceIdType.MESH
f32 = jnp.float32
bf16 = jnp.bfloat16
i32 = jnp.int32

Z = 4
G = 8
HD = 128
SUB = 48
BLK = Z * SUB
ROWS = Z * BLK
HALF = ROWS // 2
T = 256
NT = ROWS // T
TILES = range(NT)
QUAD = range(Z)
OFFS = (1, 2, 3)
NEAR = (1, 3)
SCALE = 1.0 / math.sqrt(HD)
SCALE2 = SCALE * math.log2(math.e)
NEG = -1e30
N_PAIR = 18
LAST = G - 1

KINDS = {'ka': Z, 'va': Z, 'kx': 1, 'vy': 1, 'ky': Z, 'vx': Z,
         'q': 3, 'qh': 2, 'qf': Z, 'do': 3, 'doh': 2, 'dof': Z,
         'st': Z, 'sz': Z, 'ld': Z, 'o': Z, 'oz': 1, 'g': Z, 'gz': 1,
         'rk': Z, 'rv': Z, 'sk': Z, 'sv': Z, 'fk': 2, 'fv': 2}
N_RECV = sum(KINDS.values())
N_SEND = len(KINDS) + 2 * Z


def dot(a, b, ca, cb):
    return lax.dot_general(a, b, (((ca,), (cb,)), ((), ())), preferred_element_type=f32)


def tile(n):
    return slice(n * T, (n + 1) * T)


def rem(n, k=Z):
    return n % k if isinstance(n, int) else lax.rem(n, jnp.int32(k))


def div(n, k=Z):
    return n // k if isinstance(n, int) else lax.div(n, jnp.int32(k))


def sub_rows(n):
    return pl.ds(pl.multiple_of(SUB * n, SUB), SUB)


def body(q_hbm, k_hbm, v_hbm, do_hbm, o_hbm, dq_hbm, dk_hbm, dv_hbm,
         k_loc, v_loc, q_all, do_all, k_all, v_all, kt, vt, acc, dk, dv, cache, dpb,
         m_run, l_run, st_loc, st_par, st_col, ld,
         or1, or2, dqr2, dkr1, dvr1, dkr2, dvr2, kst, vst, dk_fin, dv_fin, s_sem, r_sem, room):
    a = lax.axis_index('ctxo')
    b = lax.axis_index('ctx')
    z = div(b, Z * Z)
    y = rem(div(b))
    x = rem(b)
    m_blk = Z * y + x
    i_own = Z * a + z
    pa = 1 - a
    par = rem(a + z, 2)
    names = list(KINDS)
    base = {kind: sum(KINDS[k] for k in names[:n]) for n, kind in enumerate(names)}

    def dev(a_, z_, y_, x_):
        return {'ctxo': a_, 'ctx': Z * Z * z_ + Z * y_ + x_}

    partner = dev(pa, z, y, x)

    def col(d):
        return dev(a, rem(z + d), y, x)

    def other_col(d):
        return dev(pa, rem(z + d), y, x)

    def in_y(d):
        return dev(a, z, rem(y + d), x)

    def in_x(d):
        return dev(a, z, y, rem(x + d))

    def rc(kind, n, src, dst, to):
        return pltpu.make_async_remote_copy(src_ref=src, dst_ref=dst, send_sem=s_sem.at[names.index(kind)], recv_sem=r_sem.at[base[kind] + n],
                                            device_id=to, device_id_type=MESH)

    def send(kind, n, src, dst, to):
        rc(kind, n, src, dst, to).start()

    def got(kind, n, ref):
        rc(kind, n, ref, ref, partner).wait_recv()

    def sent(kind, ref):
        rc(kind, 0, ref, ref, partner).wait_send()

    def when(cond, fn, *args):
        pl.when(cond)(functools.partial(fn, *args))

    def group_of(s):
        a_s = div(s, 2)
        return a_s, 2 * rem(s, 2) + rem(a_s + a, 2)

    def g_of(s):
        a_s, z_s = group_of(s)
        return Z * a_s + z_s

    def not_mine(s):
        return g_of(s) != i_own

    own = [(q_hbm, q_all.at[i_own]), (do_hbm, do_all.at[i_own]), (k_hbm, k_loc), (v_hbm, v_loc)]
    own = [pltpu.make_async_copy(src, dst, s_sem.at[len(KINDS) + n]) for n, (src, dst) in enumerate(own)]
    for c in reversed(own):
        c.start()
    bar = pltpu.get_barrier_semaphore()
    peers = [partner] + [f(d) for d in OFFS for f in (col, other_col, in_y, in_x)]
    for to in peers:
        pl.semaphore_signal(bar, inc=1, device_id=to, device_id_type=MESH)
    for c in reversed(own):
        c.wait()
    pl.semaphore_wait(bar, len(peers))

    QUADS = pl.ds(0, Z)
    OTHERS = pl.ds(0, 3)
    k5 = k_all.reshape(Z, Z, Z, SUB, HD)
    v5 = v_all.reshape(Z, Z, Z, SUB, HD)

    s_me = 2 * a + div(z, 2)
    keep = par == a
    for d in QUAD:
        rows = sub_rows(rem(z + d))
        to = dev(par, rem(z + d), y, x)

        def give():
            send('ka', s_me, k_loc.at[rows], k5.at[s_me, y, x], to)
            send('va', s_me, v_loc.at[rows], v5.at[s_me, y, x], to)

        if d:
            give()
        else:
            @pl.when(keep)
            def _():
                k_all[s_me, sub_rows(m_blk), :] = k_loc[rows, :]
                v_all[s_me, sub_rows(m_blk), :] = v_loc[rows, :]
            when(jnp.logical_not(keep), give)
    send('q', 2, q_all.at[i_own], q_all.at[i_own], partner)
    send('do', 2, do_all.at[i_own], do_all.at[i_own], partner)
    dk[...] = jnp.zeros(dk.shape, f32)
    dv[...] = jnp.zeros(dv.shape, f32)

    def kv_share():
        for s in QUAD:
            @pl.when(not_mine(s))
            def _():
                got('ka', s, k5.at[s, y, x])
                got('va', s, v5.at[s, y, x])
        for d in OFFS:
            send('kx', 0, k5.at[:, y, x], k5.at[:, y, x], in_x(d))
            send('vy', 0, v5.at[:, y, x], v5.at[:, y, x], in_y(d))

    def kv_spread():
        got('kx', 0, k5.at[:, OTHERS, 0])
        got('vy', 0, v5.at[:, OTHERS, 0])
        for s in QUAD:
            for d in OFFS:
                send('ky', s, k5.at[s, y], k5.at[s, y], in_y(d))
                send('vx', s, v5.at[s, :, x], v5.at[s, :, x], in_x(d))

    def kv_ready(s):
        got('ky', s, k5.at[s, OTHERS])
        got('vx', s, v5.at[s, OTHERS])
        kt[s] = k_all[s].T
        vt[s] = v_all[s].T

    def half(ref, h):
        return ref.at[pl.ds(h * HALF, HALF)]

    def near_send(kind, full):
        for h, d in enumerate(NEAR):
            send(kind, h, full.at[i_own], full.at[i_own], col(d))

    def pass_on(kind, full, i_r, n):
        send(kind + 'f', n, full.at[i_r], full.at[i_r], partner)

    def near_got(kind, full):
        for h, d in enumerate(NEAR):
            i_r = Z * a + rem(z + Z - d)
            got(kind, h, full.at[i_r])
            pass_on(kind, full, i_r, d)
            send(kind + 'h', h, half(full.at[i_r], h), half(full.at[i_r], h), col(d))

    def far_got(kind, full):
        i_r = Z * a + rem(z + 2)
        for h in range(2):
            got(kind + 'h', h, half(full.at[i_r], h))
        pass_on(kind, full, i_r, 2)

    def passed(kind, full, d):
        i_r = Z * pa + rem(z + Z - d)
        if d:
            got(kind + 'f', d, full.at[i_r])
        else:
            got(kind, 2, full.at[i_r])

    kv_share()
    when(a == 1, near_send, 'q', q_all)
    acc[...] = jnp.zeros(acc.shape, f32)
    m_run[...] = jnp.full(m_run.shape, NEG, f32)
    l_run[...] = jnp.zeros(l_run.shape, f32)
    kv_spread()

    @pl.when(a == 1)
    def _():
        near_got('q', q_all)
        near_send('do', do_all)
    when(a == 0, near_send, 'q', q_all)

    def cache_at(i, s):
        n = i - g_of(s)
        for r in OFFS:
            n = n + (r <= s) * (G - g_of(r - 1))
        return n

    def dq_at(i):
        return jnp.where(div(i) == a, G + rem(i), i)

    def seen(j, ct):
        key_id = j * T + lax.broadcasted_iota(i32, (T, T), 0)
        pos = (ct * T + lax.broadcasted_iota(i32, (1, T), 1)) // Z
        last = SUB * m_blk + jnp.clip(pos - SUB * z, -1, SUB - 1)
        return key_id <= last

    def fold(p):
        return p.reshape(p.shape[0] // 8, 8, p.shape[1])

    def fwd_scores(i, s, pc, ct, j, mx, masked=False):
        t = dot(k_all[s, tile(j), :], q_all[i, tile(ct), :], 1, 1) * SCALE2
        if masked:
            t = jnp.where(seen(j, ct), t, -jnp.inf)
        cache[pc, tile(j), tile(ct)] = t
        r = jnp.max(fold(t), axis=0)
        return r if mx is None else jnp.maximum(mx, r)

    def fwd_first(i, s, masked=False):
        mx = None
        for j in TILES:
            mx = fwd_scores(i, s, cache_at(i, s), 0, j, mx, masked)
        return mx

    def fwd_pair(i, s, mx, i_n, s_n, pc, pc_n, masked=False):
        for ct in TILES:
            cs = tile(ct)
            last = ct == NT - 1
            nxt = (i_n, s_n, pc_n, 0) if last else (i, s, pc, ct + 1)
            m_old = m_run[i, :, cs]
            m_new = jnp.maximum(m_old, jnp.max(mx, axis=0, keepdims=True))
            al = jnp.exp2(m_old - m_new)
            mx = None
            lp = None
            o = None
            for j in TILES:
                mx = fwd_scores(*nxt, j, mx, masked and not last)
                p = jnp.exp2(cache[pc, tile(j), cs] - m_new)
                r = jnp.sum(fold(p), axis=0)
                lp = r if lp is None else lp + r
                oj = dot(vt[s, :, tile(j)], p.astype(bf16), 1, 0)
                o = oj if o is None else o + oj
            l_run[i, :, cs] = l_run[i, :, cs] * al + jnp.sum(lp, axis=0, keepdims=True)
            acc[i, :, cs] = acc[i, :, cs] * al + o
            m_run[i, :, cs] = m_new
        return mx

    def spread(lo, k):
        return lo + rem(z + k + (k >= 2) * (5 - 2 * k))

    def fwd_seg(e):
        s = rem(e)
        g = g_of(s)
        hi = jnp.where(e < Z, G, Z)
        at = cache_at(0, s)

        def plain():
            @pl.when(e == 0)
            def _():
                @pl.when(a == 0)
                def _():
                    passed('q', q_all, 0)
                    for d in NEAR:
                        passed('q', q_all, d)

            def pair(k, mx):
                when((e == 0) & (k == 1) & (a == 1), far_got, 'q', q_all)
                when((e == 0) & (k == 2) & (a == 0), passed, 'q', q_all, 2)
                i = spread(Z, k)
                i_n = spread(Z, jnp.minimum(k + 1, Z - 1))
                return fwd_pair(i, s, mx, i_n, s, at + i, at + i_n)
            lax.fori_loop(0, Z, pair, fwd_first(spread(Z, 0), s))

        def diagonal():
            more = g + 1 < hi
            mx = fwd_pair(g, s, fwd_first(g, s, True), jnp.where(more, g + 1, LAST), jnp.where(more, s, 0),
                          at + g, jnp.where(more, at + g + 1, cache_at(LAST, 0)), True)

            def pair(i, mx):
                i_n = jnp.minimum(i + 1, hi - 1)
                return fwd_pair(i, s, mx, i_n, s, at + i, at + i_n)
            lax.fori_loop(g + 1, hi, pair, mx)
        when(e < Z, kv_ready, s)
        when(e < 2, plain)
        when(e >= 2, diagonal)

    def put(ref, at, *rows):
        for n, r in enumerate(rows):
            ref[(*at, slice(n, n + 1), slice(None))] = r

    def get(ref, *at):
        return [ref[(*at, slice(n, n + 1), slice(None))] for n in range(ref.shape[-2])]

    def fwd_done(i, c):
        z_i = rem(i)
        d_part = jnp.sum(do_all[i].T.astype(f32) * acc[i], axis=0, keepdims=True)
        put(st_loc, (i,), m_run[i], l_run[i], d_part)

        @pl.when(div(i) != a)
        def _():
            send('st', z_i, st_loc.at[i], st_par.at[z_i], partner)
        return c

    def out_give():
        for n in QUAD:
            send('o', n, acc.at[Z * pa + n], or1.at[n], partner)

    def pair_done(z_o):
        i = Z * a + z_o
        got('st', z_o, st_par.at[z_o])
        mine = get(st_loc, i)
        other = get(st_par, z_o)
        top = jnp.maximum(mine[0], other[0])
        w0 = jnp.exp2(mine[0] - top)
        w1 = jnp.exp2(other[0] - top)
        put(st_col, (z_o, z), top, *[w0 * p + w1 * q for p, q in zip(mine[1:], other[1:])])
        for d in OFFS:
            send('sz', z_o, st_col.at[z_o, z], st_col.at[z_o, z], col(d))

    def out_join(z_o):
        i = Z * a + z_o
        got('o', z_o, or1.at[z_o])
        top = get(st_col, z_o, z)[0]
        w0 = jnp.exp2(get(st_loc, i)[0] - top)
        w1 = jnp.exp2(get(st_par, z_o)[0] - top)
        for ct in TILES:
            cs = tile(ct)
            acc[i, :, cs] = acc[i, :, cs] * w0[:, cs] + or1[z_o, :, cs] * w1[:, cs]
        h = rem(z_o + Z - z)

        @pl.when(h != 0)
        def _():
            send('oz', 0, acc.at[i], or2.at[h - 1], dev(a, z_o, y, x))

    def joins():
        for d in (2, 1, 3, 0):
            out_join(rem(z + d))
        pl.semaphore_signal(room, inc=1, device_id=partner, device_id_type=MESH)

    def col_done(z_o):
        i = Z * a + z_o
        got('sz', z_o, st_col.at[z_o, OTHERS])
        parts = [get(st_col, z_o, n) for n in QUAD]
        big = functools.reduce(jnp.maximum, [p[0] for p in parts])
        w = [jnp.exp2(p[0] - big) for p in parts]
        tot = sum(wn * p[1] for wn, p in zip(w, parts))
        dsum = sum(wn * p[2] for wn, p in zip(w, parts))
        put(ld, (i,), big + jnp.log(tot) * math.log2(math.e), dsum / tot)
        send('ld', z_o, ld.at[i], ld.at[i], partner)

    def passed_all(kind, full):
        for d in (0,) + OFFS:
            passed(kind, full, d)

    def seg_step(e, c):
        fwd_seg(e)

        @pl.when(a == 1)
        def _():
            when(e == 1, near_got, 'do', do_all)
            when(e == 2, far_got, 'do', do_all)

            @pl.when(e == 1)
            def _():
                for d in (0,) + NEAR:
                    passed('q', q_all, d)

            @pl.when(e == 3)
            def _():
                passed('q', q_all, 2)
                lax.fori_loop(Z, G, fwd_done, 0)
                for n in (3, 2, 1, 0):
                    pair_done(n)

            @pl.when(e == 4)
            def _():
                for n in (3, 2, 1, 0):
                    col_done(n)

            @pl.when(e == 5)
            def _():
                passed_all('do', do_all)
                lax.fori_loop(0, Z, fwd_done, 0)
                out_give()
                joins()

        @pl.when(a == 0)
        def _():
            @pl.when(e == 0)
            def _():
                near_got('q', q_all)
                near_send('do', do_all)
            when(e == 1, far_got, 'q', q_all)
            when(e == 2, near_got, 'do', do_all)

            @pl.when(e == 3)
            def _():
                passed_all('do', do_all)
                lax.fori_loop(Z, G, fwd_done, 0)

            @pl.when(e == 3)
            def _():
                out_give()
            when(e == 4, far_got, 'do', do_all)

            @pl.when(e == 5)
            def _():
                lax.fori_loop(0, Z, fwd_done, 0)
        return c
    lax.fori_loop(0, 6, seg_step, 0)

    def dq_join(z_o):
        i = G + z_o
        got('g', z_o, or1.at[z_o])
        for ct in TILES:
            cs = tile(ct)
            acc[i, :, cs] = acc[i, :, cs] + or1[z_o, :, cs]
        h = rem(z_o + Z - z)

        @pl.when(h != 0)
        def _():
            send('gz', 0, acc.at[i], dqr2.at[h - 1], dev(a, z_o, y, x))

    def dq_room():
        sent('o', or1)
        for n in QUAD:
            acc[Z * pa + n] = jnp.zeros(or1.shape[1:], f32)

    def bwd_scores(i, s, u):
        j, ct = divmod(u, NT)
        dpb[u % NT] = dot(v_all[s, tile(j), :], do_all[i, tile(ct), :], 1, 1)

    def bwd_pair(i, s, i_n, s_n, pc, dq):
        acc_v = None
        acc_k = None
        pend = None

        def products(u, p, ds, acc_v, acc_k):
            j, ct = divmod(u, NT)
            e = dot(p, do_all[i, tile(ct), :], 1, 0)
            g = dot(ds, q_all[i, tile(ct), :], 1, 0)
            acc_v = e if ct == 0 else acc_v + e
            acc_k = g if ct == 0 else acc_k + g
            acc[dq, :, tile(ct)] += dot(kt[s, :, tile(j)], ds, 1, 0)
            if ct == NT - 1:
                dv[s, tile(j), :] += acc_v
                dk[s, tile(j), :] += acc_k
            return acc_v, acc_k

        n_u = NT * NT
        for u in range(n_u):
            j, ct = divmod(u, NT)
            if u < n_u - 1:
                bwd_scores(i, s, u + 1)
            else:
                bwd_scores(i_n, s_n, 0)
            p = jnp.exp2(cache[pc, tile(j), tile(ct)] - ld[i, 0:1, tile(ct)])
            ds = p * (dpb[u % NT] - ld[i, 1:2, tile(ct)])
            now = p.astype(bf16), ds.astype(bf16)
            if pend is not None:
                acc_v, acc_k = products(u - 1, *pend, acc_v, acc_k)
            pend = now
        products(n_u - 1, *pend, acc_v, acc_k)

    def rot(k):
        return rem(z + (2, 1, 3, 0)[k])

    STEPS = 10

    def bwd_part(n):
        i, lo, hi = (LAST - n, 0, Z) if n < 4 else (n - 2, 1, 2) if n < 6 else (rot(n - 6), 0, 1)
        end = jnp.int32(0)
        for s in QUAD:
            end = end + (g_of(s) <= i).astype(i32)
        return i, lo, jnp.minimum(end, hi)

    def bwd_block(n):
        i, lo, end = bwd_part(n)
        i_n, lo_n, _ = bwd_part(min(n + 1, STEPS - 1))
        _, lo_p, end_p = bwd_part(max(n - 1, 0))

        if n == 0:
            bwd_scores(i, lo, 0)
        elif n > 4:
            when((lo < end) & (lo_p >= end_p), bwd_scores, i, lo, 0)
        dq = dq_at(i)

        def pair(s, c):
            more = s + 1 < end
            bwd_pair(i, s, jnp.where(more, i, i_n), jnp.where(more, s + 1, lo_n), cache_at(i, s), dq)
            return c
        lax.fori_loop(lo, end, pair, 0)

    dk5 = dk.reshape(Z, Z, Z, SUB, HD)
    dv5 = dv.reshape(Z, Z, Z, SUB, HD)
    dkr14 = dkr1.reshape(Z, 3, Z, SUB, HD)
    dvr14 = dvr1.reshape(Z, 3, Z, SUB, HD)

    def kv_first(s):
        for d in OFFS:
            send('rk', s, dk5.at[s, rem(y + d)], dkr14.at[s, d - 1], in_y(d))
            send('rv', s, dv5.at[s, :, rem(x + d)], dvr14.at[s, d - 1], in_x(d))

    def kv_second(s):
        got('rk', s, dkr1.at[s])
        got('rv', s, dvr1.at[s])
        rows = pl.ds(pl.multiple_of(BLK * y, BLK), BLK)
        dk[s, rows, :] = dk[s, rows, :] + sum(dkr1[s, d - 1] for d in OFFS)
        for n in QUAD:
            rows = sub_rows(Z * n + x)
            dv[s, rows, :] = dv[s, rows, :] + sum(dvr1[s, d - 1, n * SUB:(n + 1) * SUB, :] for d in OFFS)
        for d in OFFS:
            send('sk', s, dk5.at[s, y, rem(x + d)], dkr2.at[s, d - 1], in_x(d))
            send('sv', s, dv5.at[s, rem(y + d), x], dvr2.at[s, d - 1], in_y(d))

    def kv_third(s):
        got('sk', s, dkr2.at[s])
        got('sv', s, dvr2.at[s])
        kst[s] = ((dk[s, sub_rows(m_blk), :] + sum(dkr2[s, d - 1] for d in OFFS)) * SCALE).astype(bf16)
        vst[s] = (dv[s, sub_rows(m_blk), :] + sum(dvr2[s, d - 1] for d in OFFS)).astype(bf16)
        a_s, z_s = group_of(s)
        rows = sub_rows(z)

        @pl.when(g_of(s) == i_own)
        def _():
            dk_fin[rows, :] = kst[s]
            dv_fin[rows, :] = vst[s]

        @pl.when(not_mine(s))
        def _():
            to = dev(a_s, z_s, y, x)
            far = (z_s != z).astype(i32)
            send('fk', far, kst.at[s], dk_fin.at[rows], to)
            send('fv', far, vst.at[s], dv_fin.at[rows], to)

    def bwd_step(n):
        i, lo, _ = bwd_part(n)
        a_i = div(i)
        z_i = rem(i)
        to = 0 if n < 4 else 1
        mine = a == to
        if n in (0, 2):
            when(a == n // 2, dq_room)
        when(mine if n < 6 else mine & (z_i < 2), got, 'ld', z_i, ld.at[i])
        bwd_block(n)

        def give():
            send('g', z_i, acc.at[i], or1.at[z_i], partner)
        if n in (0, 6):
            when(mine, pl.semaphore_wait, room, 1)
        if lo == 0:
            when(mine, give)
        for core, firsts, seconds, thirds, joined in (
                (0, {0: 3, 2: 2, 5: 1, 9: 0}, {2: 3, 6: 2}, {}, {7: rot(0), 8: rot(1), 9: rot(2)}),
                (1, {1: 3, 3: 2, 5: 1, 9: 0}, {3: 3, 8: 2}, {}, {1: 3, 2: 2, 3: 1, 5: 0})):
            def events():
                if n in firsts:
                    kv_first(firsts[n])
                if n == 0 and core == 0:
                    for k in (2, 3, 1, 0):
                        pair_done(k)
                    joins()
                if n == 2 and core == 0:
                    for k in (2, 3, 1, 0):
                        col_done(k)
                if n in joined:
                    dq_join(joined[n])
                if n in seconds:
                    kv_second(seconds[n])
                if n in thirds:
                    kv_third(thirds[n])
            when(a == core, events)

    for n in range(STEPS):
        bwd_step(n)

    when(a == 0, dq_join, z)
    sent('kx', k5.at[:, OTHERS, 0])
    sent('ky', k5.at[OTHERS])
    outs = [(k_all.at[0], o_hbm), (k_all.at[1], dq_hbm), (dk_fin, dk_hbm), (dv_fin, dv_hbm)]
    outs = [pltpu.make_async_copy(src, dst, s_sem.at[len(KINDS) + Z + n]) for n, (src, dst) in enumerate(outs)]
    got('oz', 0, or2)
    w_z = [jnp.exp2(get(st_col, z, rem(z + Z - h))[0] - ld[i_own, 0:1, :]) for h in QUAD]
    for ct in TILES:
        cs = tile(ct)
        o = acc[i_own, :, cs] * w_z[0][:, cs]
        for h in OFFS:
            o = o + or2[h - 1, :, cs] * w_z[h][:, cs]
        k_all[0, cs, :] = o.T.astype(bf16)
    outs[0].start()

    def left(n):
        sent('ka', k_loc.at[pl.ds(0, n * SUB)])
        sent('va', v_loc.at[pl.ds(0, n * SUB)])
    when(keep, left, 3)
    when(jnp.logical_not(keep), left, Z)
    for kind, full in (('q', q_all), ('do', do_all)):
        sent(kind, full.at[OTHERS])
        sent(kind + 'h', full.at[0])
        sent(kind + 'f', full.at[OTHERS])
    for kind, ref in (('vy', v5.at[:, OTHERS, 0]), ('vx', v5.at[OTHERS]), ('st', st_par), ('ld', ld.at[QUADS]), ('oz', or2), ('sz', st_col.at[:, OTHERS])):
        sent(kind, ref)
    kv_third(3)
    kv_second(1)
    kv_third(2)
    kv_second(0)
    kv_third(1)
    got('gz', 0, dqr2)
    for ct in TILES:
        cs = tile(ct)
        k_all[1, cs, :] = ((acc[G + z, :, cs] + sum(dqr2[h - 1, :, cs] for h in OFFS)).T * SCALE).astype(bf16)
    outs[1].start()
    kv_third(0)
    def take(n, rows):
        got('fk', n, dk_fin.at[rows])
        got('fv', n, dv_fin.at[rows])
    take(1, pl.ds(0, BLK - SUB))
    when(jnp.logical_not(keep), take, 0, pl.ds(0, SUB))
    outs[2].start()
    outs[3].start()

    for kind, ref in (('g', or1), ('gz', dqr2), ('rk', dkr1), ('rv', dvr1), ('sk', dkr2), ('sv', dvr2)):
        sent(kind, ref)

    def back(n):
        sent('fk', kst.at[pl.ds(0, n)])
        sent('fv', vst.at[pl.ds(0, n)])
    when(keep, back, 3)
    when(jnp.logical_not(keep), back, Z)
    for c in outs:
        c.wait()


def solution(mesh):
    blk_spec = P('data', CTX_AXES, None, None)
    v = pltpu.VMEM
    big = (ROWS, HD)
    big_t = (HD, ROWS)
    blk = (BLK, HD)
    sub = (SUB, HD)
    scratch = [
        *[v(blk, bf16)] * 2,
        *[v((G,) + big, bf16)] * 2, *[v((Z,) + big, bf16)] * 2,
        *[v((Z,) + big_t, bf16)] * 2,
        v((G + Z,) + big_t, f32), *[v((Z,) + big, f32)] * 2,
        v((N_PAIR, ROWS, ROWS), f32),
        v((NT, T, T), f32),
        *[v((G, 1, ROWS), f32)] * 2, v((G, 3, ROWS), f32),
        v((Z, 3, ROWS), f32), v((Z, Z, 3, ROWS), f32), v((G, 2, ROWS), f32),
        v((Z,) + big_t, f32), *[v((3,) + big_t, f32)] * 2,
        *[v((Z, 3) + blk, f32)] * 2,
        *[v((Z, 3) + sub, f32)] * 2, *[v((Z,) + sub, bf16)] * 2,
        *[v(blk, bf16)] * 2,
        pltpu.SemaphoreType.DMA((N_SEND,)), pltpu.SemaphoreType.DMA((N_RECV,)), pltpu.SemaphoreType.REGULAR,
    ]
    call = pl.pallas_call(
        body,
        name='attn',
        out_shape=[jax.ShapeDtypeStruct(big, bf16)] * 2 + [jax.ShapeDtypeStruct(blk, bf16)] * 2,
        in_specs=[pl.BlockSpec(memory_space=pl.ANY)] * 4,
        out_specs=[pl.BlockSpec(memory_space=pl.ANY)] * 4,
        scratch_shapes=scratch,
        compiler_params=pltpu.CompilerParams(collective_id=0, has_side_effects=True, vmem_limit_bytes=67043328),
    )

    def hand_out(*refs):
        srcs, dsts, bufs, sems = refs[:Z], refs[Z:2 * Z], refs[2 * Z:3 * Z], refs[3 * Z]
        ins = [pltpu.make_async_copy(src, buf, sems.at[0, n]) for n, (src, buf) in enumerate(zip(srcs, bufs))]
        outs = [pltpu.make_async_copy(buf, dst, sems.at[1, n]) for n, (buf, dst) in enumerate(zip(bufs, dsts))]
        for c in ins:
            c.start()
        for c, e in zip(ins, outs):
            c.wait()
            e.start()
        for e in outs:
            e.wait()

    leave = pl.pallas_call(
        hand_out,
        name='leave',
        out_shape=[jax.ShapeDtypeStruct(big, bf16)] * 2 + [jax.ShapeDtypeStruct(blk, bf16)] * 2,
        in_specs=[pl.BlockSpec(memory_space=pl.ANY)] * 4,
        out_specs=[pl.BlockSpec(memory_space=pl.ANY)] * 4,
        scratch_shapes=[*[v(big, bf16)] * 2, *[v(blk, bf16)] * 2, pltpu.SemaphoreType.DMA((2, Z))],
    )

    def local_attn(q_in, k_in, v_in, do_in):
        o, dq, dk, dv = leave(*call(q_in.reshape(big), k_in.reshape(blk), v_in.reshape(blk), do_in.reshape(big)))
        return o.reshape(q_in.shape), dq.reshape(q_in.shape), dk.reshape(k_in.shape), dv.reshape(k_in.shape)

    return jax.shard_map(local_attn, mesh=mesh, in_specs=(blk_spec,) * 4, out_specs=(blk_spec,) * 4, check_vma=False)
```

```python
import functools
import math
import jax
import jax.numpy as jnp
from jax import lax
from jax.experimental import pallas as pl
from jax.experimental.pallas import tpu as pltpu
from jax.sharding import PartitionSpec as P

CTX_AXES = ('ctxo', 'ctx')
MESH = pl.DeviceIdType.MESH
f32 = jnp.float32
bf16 = jnp.bfloat16
i32 = jnp.int32

Z = 4
G = 8
HD = 128
SUB = 48
BLK = Z * SUB
ROWS = Z * BLK
HALF = ROWS // 2
T = 256
NT = ROWS // T
TILES = range(NT)
QUAD = range(Z)
OFFS = (1, 2, 3)
NEAR = (1, 3)
SCALE = 1.0 / math.sqrt(HD)
SCALE2 = SCALE * math.log2(math.e)
NEG = -1e30
N_PAIR = 18
LAST = G - 1

KINDS = {'ka': Z, 'va': Z, 'kx': 1, 'vy': 1, 'ky': Z, 'vx': Z,
         'q': 3, 'qh': 2, 'qf': Z, 'do': 3, 'doh': 2, 'dof': Z,
         'st': Z, 'sz': Z, 'ld': Z, 'o': Z, 'oz': 1, 'g': Z, 'gz': 1,
         'rk': Z, 'rv': Z, 'sk': Z, 'sv': Z, 'fk': 2, 'fv': 2}
N_RECV = sum(KINDS.values())
N_SEND = len(KINDS) + Z


def dot(a, b, ca, cb):
    return lax.dot_general(a, b, (((ca,), (cb,)), ((), ())), preferred_element_type=f32)


def tile(n):
    return slice(n * T, (n + 1) * T)


def rem(n, k=Z):
    return n % k if isinstance(n, int) else lax.rem(n, jnp.int32(k))


def div(n, k=Z):
    return n // k if isinstance(n, int) else lax.div(n, jnp.int32(k))


def sub_rows(n):
    return pl.ds(pl.multiple_of(SUB * n, SUB), SUB)


def body(q_hbm, k_hbm, v_hbm, do_hbm, o_out, dq_out, dk_out, dv_out,
         k_loc, v_loc, q_all, do_all, k_all, v_all, kt, vt, acc, dk, dv, cache, dpb,
         m_run, l_run, st_loc, st_par, st_col, ld,
         or1, or2, dqr2, dkr1, dvr1, dkr2, dvr2, kst, vst, dk_fin, dv_fin, s_sem, r_sem, room):
    a = lax.axis_index('ctxo')
    b = lax.axis_index('ctx')
    z = div(b, Z * Z)
    y = rem(div(b))
    x = rem(b)
    m_blk = Z * y + x
    i_own = Z * a + z
    pa = 1 - a
    par = rem(a + z, 2)
    names = list(KINDS)
    base = {kind: sum(KINDS[k] for k in names[:n]) for n, kind in enumerate(names)}

    def dev(a_, z_, y_, x_):
        return {'ctxo': a_, 'ctx': Z * Z * z_ + Z * y_ + x_}

    partner = dev(pa, z, y, x)

    def col(d):
        return dev(a, rem(z + d), y, x)

    def other_col(d):
        return dev(pa, rem(z + d), y, x)

    def in_y(d):
        return dev(a, z, rem(y + d), x)

    def in_x(d):
        return dev(a, z, y, rem(x + d))

    def rc(kind, n, src, dst, to):
        return pltpu.make_async_remote_copy(src_ref=src, dst_ref=dst, send_sem=s_sem.at[names.index(kind)], recv_sem=r_sem.at[base[kind] + n],
                                            device_id=to, device_id_type=MESH)

    def send(kind, n, src, dst, to):
        rc(kind, n, src, dst, to).start()

    def got(kind, n, ref):
        rc(kind, n, ref, ref, partner).wait_recv()

    def sent(kind, ref):
        rc(kind, 0, ref, ref, partner).wait_send()

    def when(cond, fn, *args):
        pl.when(cond)(functools.partial(fn, *args))

    def group_of(s):
        a_s = div(s, 2)
        return a_s, 2 * rem(s, 2) + rem(a_s + a, 2)

    def g_of(s):
        a_s, z_s = group_of(s)
        return Z * a_s + z_s

    def not_mine(s):
        return g_of(s) != i_own

    own = [(q_hbm, q_all.at[i_own]), (do_hbm, do_all.at[i_own]), (k_hbm, k_loc), (v_hbm, v_loc)]
    own = [pltpu.make_async_copy(src, dst, s_sem.at[len(KINDS) + n]) for n, (src, dst) in enumerate(own)]
    for c in reversed(own):
        c.start()
    bar = pltpu.get_barrier_semaphore()
    peers = [partner] + [f(d) for d in OFFS for f in (col, other_col, in_y, in_x)]
    for to in peers:
        pl.semaphore_signal(bar, inc=1, device_id=to, device_id_type=MESH)
    for c in reversed(own):
        c.wait()
    pl.semaphore_wait(bar, len(peers))

    QUADS = pl.ds(0, Z)
    OTHERS = pl.ds(0, 3)
    k5 = k_all.reshape(Z, Z, Z, SUB, HD)
    v5 = v_all.reshape(Z, Z, Z, SUB, HD)

    s_me = 2 * a + div(z, 2)
    keep = par == a
    for d in QUAD:
        rows = sub_rows(rem(z + d))
        to = dev(par, rem(z + d), y, x)

        def give():
            send('ka', s_me, k_loc.at[rows], k5.at[s_me, y, x], to)
            send('va', s_me, v_loc.at[rows], v5.at[s_me, y, x], to)

        if d:
            give()
        else:
            @pl.when(keep)
            def _():
                k_all[s_me, sub_rows(m_blk), :] = k_loc[rows, :]
                v_all[s_me, sub_rows(m_blk), :] = v_loc[rows, :]
            when(jnp.logical_not(keep), give)
    send('q', 2, q_all.at[i_own], q_all.at[i_own], partner)
    send('do', 2, do_all.at[i_own], do_all.at[i_own], partner)
    dk[...] = jnp.zeros(dk.shape, f32)
    dv[...] = jnp.zeros(dv.shape, f32)

    def kv_share():
        for s in QUAD:
            @pl.when(not_mine(s))
            def _():
                got('ka', s, k5.at[s, y, x])
                got('va', s, v5.at[s, y, x])
        for d in OFFS:
            send('kx', 0, k5.at[:, y, x], k5.at[:, y, x], in_x(d))
            send('vy', 0, v5.at[:, y, x], v5.at[:, y, x], in_y(d))

    def kv_spread():
        got('kx', 0, k5.at[:, OTHERS, 0])
        got('vy', 0, v5.at[:, OTHERS, 0])
        for s in QUAD:
            for d in OFFS:
                send('ky', s, k5.at[s, y], k5.at[s, y], in_y(d))
                send('vx', s, v5.at[s, :, x], v5.at[s, :, x], in_x(d))

    def kv_ready(s):
        got('ky', s, k5.at[s, OTHERS])
        got('vx', s, v5.at[s, OTHERS])
        kt[s] = k_all[s].T
        vt[s] = v_all[s].T

    def half(ref, h):
        return ref.at[pl.ds(h * HALF, HALF)]

    def near_send(kind, full):
        for h, d in enumerate(NEAR):
            send(kind, h, full.at[i_own], full.at[i_own], col(d))

    def pass_on(kind, full, i_r, n):
        send(kind + 'f', n, full.at[i_r], full.at[i_r], partner)

    def near_got(kind, full):
        for h, d in enumerate(NEAR):
            i_r = Z * a + rem(z + Z - d)
            got(kind, h, full.at[i_r])
            pass_on(kind, full, i_r, d)
            send(kind + 'h', h, half(full.at[i_r], h), half(full.at[i_r], h), col(d))

    def far_got(kind, full):
        i_r = Z * a + rem(z + 2)
        for h in range(2):
            got(kind + 'h', h, half(full.at[i_r], h))
        pass_on(kind, full, i_r, 2)

    def passed(kind, full, d):
        i_r = Z * pa + rem(z + Z - d)
        if d:
            got(kind + 'f', d, full.at[i_r])
        else:
            got(kind, 2, full.at[i_r])

    kv_share()
    when(a == 1, near_send, 'q', q_all)
    acc[...] = jnp.zeros(acc.shape, f32)
    m_run[...] = jnp.full(m_run.shape, NEG, f32)
    l_run[...] = jnp.zeros(l_run.shape, f32)
    kv_spread()

    @pl.when(a == 1)
    def _():
        near_got('q', q_all)
        near_send('do', do_all)
    when(a == 0, near_send, 'q', q_all)

    def cache_at(i, s):
        n = i - g_of(s)
        for r in OFFS:
            n = n + (r <= s) * (G - g_of(r - 1))
        return n

    def dq_at(i):
        return jnp.where(div(i) == a, G + rem(i), i)

    def seen(j, ct):
        key_id = j * T + lax.broadcasted_iota(i32, (T, T), 0)
        pos = (ct * T + lax.broadcasted_iota(i32, (1, T), 1)) // Z
        last = SUB * m_blk + jnp.clip(pos - SUB * z, -1, SUB - 1)
        return key_id <= last

    def fold(p):
        return p.reshape(p.shape[0] // 8, 8, p.shape[1])

    def fwd_scores(i, s, pc, ct, j, mx, masked=False):
        t = dot(k_all[s, tile(j), :], q_all[i, tile(ct), :], 1, 1) * SCALE2
        if masked:
            t = jnp.where(seen(j, ct), t, -jnp.inf)
        cache[pc, tile(j), tile(ct)] = t
        r = jnp.max(fold(t), axis=0)
        return r if mx is None else jnp.maximum(mx, r)

    def fwd_first(i, s, masked=False):
        mx = None
        for j in TILES:
            mx = fwd_scores(i, s, cache_at(i, s), 0, j, mx, masked)
        return mx

    def fwd_pair(i, s, mx, i_n, s_n, pc, pc_n, masked=False):
        for ct in TILES:
            cs = tile(ct)
            last = ct == NT - 1
            nxt = (i_n, s_n, pc_n, 0) if last else (i, s, pc, ct + 1)
            m_old = m_run[i, :, cs]
            m_new = jnp.maximum(m_old, jnp.max(mx, axis=0, keepdims=True))
            al = jnp.exp2(m_old - m_new)
            mx = None
            lp = None
            o = None
            for j in TILES:
                mx = fwd_scores(*nxt, j, mx, masked and not last)
                p = jnp.exp2(cache[pc, tile(j), cs] - m_new)
                r = jnp.sum(fold(p), axis=0)
                lp = r if lp is None else lp + r
                oj = dot(vt[s, :, tile(j)], p.astype(bf16), 1, 0)
                o = oj if o is None else o + oj
            l_run[i, :, cs] = l_run[i, :, cs] * al + jnp.sum(lp, axis=0, keepdims=True)
            acc[i, :, cs] = acc[i, :, cs] * al + o
            m_run[i, :, cs] = m_new
        return mx

    def spread(lo, k):
        return lo + rem(z + k + (k >= 2) * (5 - 2 * k))

    def fwd_seg(e):
        s = rem(e)
        g = g_of(s)
        hi = jnp.where(e < Z, G, Z)
        at = cache_at(0, s)

        def plain():
            @pl.when(e == 0)
            def _():
                @pl.when(a == 0)
                def _():
                    passed('q', q_all, 0)
                    for d in NEAR:
                        passed('q', q_all, d)

            def pair(k, mx):
                when((e == 0) & (k == 1) & (a == 1), far_got, 'q', q_all)
                when((e == 0) & (k == 2) & (a == 0), passed, 'q', q_all, 2)
                i = spread(Z, k)
                i_n = spread(Z, jnp.minimum(k + 1, Z - 1))
                return fwd_pair(i, s, mx, i_n, s, at + i, at + i_n)
            lax.fori_loop(0, Z, pair, fwd_first(spread(Z, 0), s))

        def diagonal():
            more = g + 1 < hi
            mx = fwd_pair(g, s, fwd_first(g, s, True), jnp.where(more, g + 1, LAST), jnp.where(more, s, 0),
                          at + g, jnp.where(more, at + g + 1, cache_at(LAST, 0)), True)

            def pair(i, mx):
                i_n = jnp.minimum(i + 1, hi - 1)
                return fwd_pair(i, s, mx, i_n, s, at + i, at + i_n)
            lax.fori_loop(g + 1, hi, pair, mx)
        when(e < Z, kv_ready, s)
        when(e < 2, plain)
        when(e >= 2, diagonal)

    def put(ref, at, *rows):
        for n, r in enumerate(rows):
            ref[(*at, slice(n, n + 1), slice(None))] = r

    def get(ref, *at):
        return [ref[(*at, slice(n, n + 1), slice(None))] for n in range(ref.shape[-2])]

    def fwd_done(i, c):
        z_i = rem(i)
        d_part = jnp.sum(do_all[i].T.astype(f32) * acc[i], axis=0, keepdims=True)
        put(st_loc, (i,), m_run[i], l_run[i], d_part)

        @pl.when(div(i) != a)
        def _():
            send('st', z_i, st_loc.at[i], st_par.at[z_i], partner)
        return c

    def out_give():
        for n in QUAD:
            send('o', n, acc.at[Z * pa + n], or1.at[n], partner)

    def pair_done(z_o):
        i = Z * a + z_o
        got('st', z_o, st_par.at[z_o])
        mine = get(st_loc, i)
        other = get(st_par, z_o)
        top = jnp.maximum(mine[0], other[0])
        w0 = jnp.exp2(mine[0] - top)
        w1 = jnp.exp2(other[0] - top)
        put(st_col, (z_o, z), top, *[w0 * p + w1 * q for p, q in zip(mine[1:], other[1:])])
        for d in OFFS:
            send('sz', z_o, st_col.at[z_o, z], st_col.at[z_o, z], col(d))

    def out_join(z_o):
        i = Z * a + z_o
        got('o', z_o, or1.at[z_o])
        top = get(st_col, z_o, z)[0]
        w0 = jnp.exp2(get(st_loc, i)[0] - top)
        w1 = jnp.exp2(get(st_par, z_o)[0] - top)
        for ct in TILES:
            cs = tile(ct)
            acc[i, :, cs] = acc[i, :, cs] * w0[:, cs] + or1[z_o, :, cs] * w1[:, cs]
        h = rem(z_o + Z - z)

        @pl.when(h != 0)
        def _():
            send('oz', 0, acc.at[i], or2.at[h - 1], dev(a, z_o, y, x))

    def joins():
        for d in (2, 1, 3, 0):
            out_join(rem(z + d))
        pl.semaphore_signal(room, inc=1, device_id=partner, device_id_type=MESH)

    def col_done(z_o):
        i = Z * a + z_o
        got('sz', z_o, st_col.at[z_o, OTHERS])
        parts = [get(st_col, z_o, n) for n in QUAD]
        big = functools.reduce(jnp.maximum, [p[0] for p in parts])
        w = [jnp.exp2(p[0] - big) for p in parts]
        tot = sum(wn * p[1] for wn, p in zip(w, parts))
        dsum = sum(wn * p[2] for wn, p in zip(w, parts))
        put(ld, (i,), big + jnp.log(tot) * math.log2(math.e), dsum / tot)
        send('ld', z_o, ld.at[i], ld.at[i], partner)

    def passed_all(kind, full):
        for d in (0,) + OFFS:
            passed(kind, full, d)

    def seg_step(e, c):
        fwd_seg(e)

        @pl.when(a == 1)
        def _():
            when(e == 1, near_got, 'do', do_all)
            when(e == 2, far_got, 'do', do_all)

            @pl.when(e == 1)
            def _():
                for d in (0,) + NEAR:
                    passed('q', q_all, d)

            @pl.when(e == 3)
            def _():
                passed('q', q_all, 2)
                lax.fori_loop(Z, G, fwd_done, 0)
                for n in (3, 2, 1, 0):
                    pair_done(n)

            @pl.when(e == 4)
            def _():
                for n in (3, 2, 1, 0):
                    col_done(n)

            @pl.when(e == 5)
            def _():
                passed_all('do', do_all)
                lax.fori_loop(0, Z, fwd_done, 0)
                out_give()
                joins()

        @pl.when(a == 0)
        def _():
            @pl.when(e == 0)
            def _():
                near_got('q', q_all)
                near_send('do', do_all)
            when(e == 1, far_got, 'q', q_all)
            when(e == 2, near_got, 'do', do_all)

            @pl.when(e == 3)
            def _():
                passed_all('do', do_all)
                lax.fori_loop(Z, G, fwd_done, 0)

            @pl.when(e == 3)
            def _():
                out_give()
            when(e == 4, far_got, 'do', do_all)

            @pl.when(e == 5)
            def _():
                lax.fori_loop(0, Z, fwd_done, 0)
        return c
    lax.fori_loop(0, 6, seg_step, 0)

    def dq_join(z_o):
        i = G + z_o
        got('g', z_o, or1.at[z_o])
        for ct in TILES:
            cs = tile(ct)
            acc[i, :, cs] = acc[i, :, cs] + or1[z_o, :, cs]
        h = rem(z_o + Z - z)

        @pl.when(h != 0)
        def _():
            send('gz', 0, acc.at[i], dqr2.at[h - 1], dev(a, z_o, y, x))

    def dq_room():
        sent('o', or1)
        for n in QUAD:
            acc[Z * pa + n] = jnp.zeros(or1.shape[1:], f32)

    def bwd_scores(i, s, u):
        j, ct = divmod(u, NT)
        dpb[u % NT] = dot(v_all[s, tile(j), :], do_all[i, tile(ct), :], 1, 1)

    def bwd_pair(i, s, i_n, s_n, pc, dq):
        acc_v = None
        acc_k = None
        pend = None

        def products(u, p, ds, acc_v, acc_k):
            j, ct = divmod(u, NT)
            e = dot(p, do_all[i, tile(ct), :], 1, 0)
            g = dot(ds, q_all[i, tile(ct), :], 1, 0)
            acc_v = e if ct == 0 else acc_v + e
            acc_k = g if ct == 0 else acc_k + g
            acc[dq, :, tile(ct)] += dot(kt[s, :, tile(j)], ds, 1, 0)
            if ct == NT - 1:
                dv[s, tile(j), :] += acc_v
                dk[s, tile(j), :] += acc_k
            return acc_v, acc_k

        n_u = NT * NT
        for u in range(n_u):
            j, ct = divmod(u, NT)
            if u < n_u - 1:
                bwd_scores(i, s, u + 1)
            else:
                bwd_scores(i_n, s_n, 0)
            p = jnp.exp2(cache[pc, tile(j), tile(ct)] - ld[i, 0:1, tile(ct)])
            ds = p * (dpb[u % NT] - ld[i, 1:2, tile(ct)])
            now = p.astype(bf16), ds.astype(bf16)
            if pend is not None:
                acc_v, acc_k = products(u - 1, *pend, acc_v, acc_k)
            pend = now
        products(n_u - 1, *pend, acc_v, acc_k)

    def rot(k):
        return rem(z + (2, 1, 3, 0)[k])

    STEPS = 10

    def bwd_part(n):
        i, lo, hi = (LAST - n, 0, Z) if n < 4 else (n - 2, 1, 2) if n < 6 else (rot(n - 6), 0, 1)
        end = jnp.int32(0)
        for s in QUAD:
            end = end + (g_of(s) <= i).astype(i32)
        return i, lo, jnp.minimum(end, hi)

    def bwd_block(n):
        i, lo, end = bwd_part(n)
        i_n, lo_n, _ = bwd_part(min(n + 1, STEPS - 1))
        _, lo_p, end_p = bwd_part(max(n - 1, 0))

        if n == 0:
            bwd_scores(i, lo, 0)
        elif n > 4:
            when((lo < end) & (lo_p >= end_p), bwd_scores, i, lo, 0)
        dq = dq_at(i)

        def pair(s, c):
            more = s + 1 < end
            bwd_pair(i, s, jnp.where(more, i, i_n), jnp.where(more, s + 1, lo_n), cache_at(i, s), dq)
            return c
        lax.fori_loop(lo, end, pair, 0)

    dk5 = dk.reshape(Z, Z, Z, SUB, HD)
    dv5 = dv.reshape(Z, Z, Z, SUB, HD)
    dkr14 = dkr1.reshape(Z, 3, Z, SUB, HD)
    dvr14 = dvr1.reshape(Z, 3, Z, SUB, HD)

    def kv_first(s):
        for d in OFFS:
            send('rk', s, dk5.at[s, rem(y + d)], dkr14.at[s, d - 1], in_y(d))
            send('rv', s, dv5.at[s, :, rem(x + d)], dvr14.at[s, d - 1], in_x(d))

    def kv_second(s):
        got('rk', s, dkr1.at[s])
        got('rv', s, dvr1.at[s])
        rows = pl.ds(pl.multiple_of(BLK * y, BLK), BLK)
        dk[s, rows, :] = dk[s, rows, :] + sum(dkr1[s, d - 1] for d in OFFS)
        for n in QUAD:
            rows = sub_rows(Z * n + x)
            dv[s, rows, :] = dv[s, rows, :] + sum(dvr1[s, d - 1, n * SUB:(n + 1) * SUB, :] for d in OFFS)
        for d in OFFS:
            send('sk', s, dk5.at[s, y, rem(x + d)], dkr2.at[s, d - 1], in_x(d))
            send('sv', s, dv5.at[s, rem(y + d), x], dvr2.at[s, d - 1], in_y(d))

    def kv_third(s):
        got('sk', s, dkr2.at[s])
        got('sv', s, dvr2.at[s])
        kst[s] = ((dk[s, sub_rows(m_blk), :] + sum(dkr2[s, d - 1] for d in OFFS)) * SCALE).astype(bf16)
        vst[s] = (dv[s, sub_rows(m_blk), :] + sum(dvr2[s, d - 1] for d in OFFS)).astype(bf16)
        a_s, z_s = group_of(s)
        rows = sub_rows(z)

        @pl.when(g_of(s) == i_own)
        def _():
            dk_fin[rows, :] = kst[s]
            dv_fin[rows, :] = vst[s]

        @pl.when(not_mine(s))
        def _():
            to = dev(a_s, z_s, y, x)
            far = (z_s != z).astype(i32)
            send('fk', far, kst.at[s], dk_fin.at[rows], to)
            send('fv', far, vst.at[s], dv_fin.at[rows], to)

    def bwd_step(n):
        i, lo, _ = bwd_part(n)
        a_i = div(i)
        z_i = rem(i)
        to = 0 if n < 4 else 1
        mine = a == to
        if n in (0, 2):
            when(a == n // 2, dq_room)
        when(mine if n < 6 else mine & (z_i < 2), got, 'ld', z_i, ld.at[i])
        bwd_block(n)

        def give():
            send('g', z_i, acc.at[i], or1.at[z_i], partner)
        if n in (0, 6):
            when(mine, pl.semaphore_wait, room, 1)
        if lo == 0:
            when(mine, give)
        for core, firsts, seconds, thirds, joined in (
                (0, {0: 3, 2: 2, 5: 1, 9: 0}, {2: 3, 6: 2}, {}, {7: rot(0), 8: rot(1), 9: rot(2)}),
                (1, {1: 3, 3: 2, 5: 1, 9: 0}, {3: 3, 8: 2}, {}, {1: 3, 2: 2, 3: 1, 5: 0})):
            def events():
                if n in firsts:
                    kv_first(firsts[n])
                if n == 0 and core == 0:
                    for k in (2, 3, 1, 0):
                        pair_done(k)
                    joins()
                if n == 2 and core == 0:
                    for k in (2, 3, 1, 0):
                        col_done(k)
                if n in joined:
                    dq_join(joined[n])
                if n in seconds:
                    kv_second(seconds[n])
                if n in thirds:
                    kv_third(thirds[n])
            when(a == core, events)

    for n in range(STEPS):
        bwd_step(n)

    when(a == 0, dq_join, z)
    sent('kx', k5.at[:, OTHERS, 0])
    sent('ky', k5.at[OTHERS])
    got('oz', 0, or2)
    w_z = [jnp.exp2(get(st_col, z, rem(z + Z - h))[0] - ld[i_own, 0:1, :]) for h in QUAD]
    for ct in TILES:
        cs = tile(ct)
        o = acc[i_own, :, cs] * w_z[0][:, cs]
        for h in OFFS:
            o = o + or2[h - 1, :, cs] * w_z[h][:, cs]
        o_out[cs, :] = o.T.astype(bf16)

    def left(n):
        sent('ka', k_loc.at[pl.ds(0, n * SUB)])
        sent('va', v_loc.at[pl.ds(0, n * SUB)])
    when(keep, left, 3)
    when(jnp.logical_not(keep), left, Z)
    for kind, full in (('q', q_all), ('do', do_all)):
        sent(kind, full.at[OTHERS])
        sent(kind + 'h', full.at[0])
        sent(kind + 'f', full.at[OTHERS])
    for kind, ref in (('vy', v5.at[:, OTHERS, 0]), ('vx', v5.at[OTHERS]), ('st', st_par), ('ld', ld.at[QUADS]), ('oz', or2), ('sz', st_col.at[:, OTHERS])):
        sent(kind, ref)
    kv_third(3)
    kv_second(1)
    kv_third(2)
    kv_second(0)
    kv_third(1)
    got('gz', 0, dqr2)
    for ct in TILES:
        cs = tile(ct)
        dq_out[cs, :] = ((acc[G + z, :, cs] + sum(dqr2[h - 1, :, cs] for h in OFFS)).T * SCALE).astype(bf16)
    kv_third(0)
    def take(n, rows):
        got('fk', n, dk_fin.at[rows])
        got('fv', n, dv_fin.at[rows])
    take(1, pl.ds(0, BLK - SUB))
    when(jnp.logical_not(keep), take, 0, pl.ds(0, SUB))
    dk_out[...] = dk_fin[...]
    dv_out[...] = dv_fin[...]

    for kind, ref in (('g', or1), ('gz', dqr2), ('rk', dkr1), ('rv', dvr1), ('sk', dkr2), ('sv', dvr2)):
        sent(kind, ref)

    def back(n):
        sent('fk', kst.at[pl.ds(0, n)])
        sent('fv', vst.at[pl.ds(0, n)])
    when(keep, back, 3)
    when(jnp.logical_not(keep), back, Z)


def solution(mesh):
    blk_spec = P('data', CTX_AXES, None, None)
    v = pltpu.VMEM
    big = (ROWS, HD)
    big_t = (HD, ROWS)
    blk = (BLK, HD)
    sub = (SUB, HD)
    scratch = [
        *[v(blk, bf16)] * 2,
        *[v((G,) + big, bf16)] * 2, *[v((Z,) + big, bf16)] * 2,
        *[v((Z,) + big_t, bf16)] * 2,
        v((G + Z,) + big_t, f32), *[v((Z,) + big, f32)] * 2,
        v((N_PAIR, ROWS, ROWS), f32),
        v((NT, T, T), f32),
        *[v((G, 1, ROWS), f32)] * 2, v((G, 3, ROWS), f32),
        v((Z, 3, ROWS), f32), v((Z, Z, 3, ROWS), f32), v((G, 2, ROWS), f32),
        v((Z,) + big_t, f32), *[v((3,) + big_t, f32)] * 2,
        *[v((Z, 3) + blk, f32)] * 2,
        *[v((Z, 3) + sub, f32)] * 2, *[v((Z,) + sub, bf16)] * 2,
        *[v(blk, bf16)] * 2,
        pltpu.SemaphoreType.DMA((N_SEND,)), pltpu.SemaphoreType.DMA((N_RECV,)), pltpu.SemaphoreType.REGULAR,
    ]
    call = pl.pallas_call(
        body,
        name='attn',
        out_shape=[v(big, bf16), v(big, bf16), v(blk, bf16), v(blk, bf16)],
        in_specs=[pl.BlockSpec(memory_space=pl.ANY)] * 4,
        out_specs=[pl.BlockSpec(memory_space=pltpu.VMEM)] * 4,
        scratch_shapes=scratch,
        compiler_params=pltpu.CompilerParams(collective_id=0, has_side_effects=True, vmem_limit_bytes=66519040),
    )

    def hand_out(*refs):
        outs = [pltpu.make_async_copy(src, dst, refs[-1].at[n]) for n, (src, dst) in enumerate(zip(refs[:Z], refs[Z:2 * Z]))]
        for c in outs:
            c.start()
        for c in outs:
            c.wait()

    leave = pl.pallas_call(
        hand_out,
        name='leave',
        out_shape=[jax.ShapeDtypeStruct(big, bf16)] * 2 + [jax.ShapeDtypeStruct(blk, bf16)] * 2,
        in_specs=[pl.BlockSpec(memory_space=pltpu.VMEM)] * 4,
        out_specs=[pl.BlockSpec(memory_space=pl.ANY)] * 4,
        scratch_shapes=[pltpu.SemaphoreType.DMA((Z,))],
    )

    def local_attn(q_in, k_in, v_in, do_in):
        kept = call(q_in.reshape(big), k_in.reshape(blk), v_in.reshape(blk), do_in.reshape(big))
        o, dq, dk, dv = leave(*[pltpu.with_memory_space_constraint(t, pltpu.VMEM) for t in kept])
        return o.reshape(q_in.shape), dq.reshape(q_in.shape), dk.reshape(k_in.shape), dv.reshape(k_in.shape)

    return jax.shard_map(local_attn, mesh=mesh, in_specs=(blk_spec,) * 4, out_specs=(blk_spec,) * 4, check_vma=False)
```
